256 devices in a mesh: shot: 64 (over y, z, core), grp: 4 (over x).
Axes of the slice: x: 4, y: 4, z: 8, core: 2. Of those that a mesh axis runs over, the one named last changes fastest.
Arguments:
- offsets: bfloat16 [49152, 32, 512], P(('shot', 'grp')), may hold values from -500 to 500
- slant_weights: bfloat16 [64, 32], replicated, may hold values from -1 to 1
- live: int32 [49152, 64], P(('shot', 'grp')), may hold values from 0 to 1, as said below
- block_tile: int32 [24576, 1], P(('shot', 'grp')), may hold values from 0 to 63; in each aligned block of 96 rows (0 to 95, 96 to 191, ...) at most 2 rows name the same one
- image_slot: int32 [24576], P(('shot', 'grp')), may hold values from 0 to 15
Outputs:
- image: bfloat16 [1024, 128, 512], P(('shot', 'grp'))
The draws below stay inside these ranges and needn't reach their ends.
Inputs may be any that keep to these rules, and one draw needn't show every extreme that they name: Each position's live angles are 0 up to a cutoff minus 1, the cutoff at least 16; the first position of every 192 positions keeps all 64 angles. `block_tile`: among the 96 blocks of one device no tile is named more than 2 times.
All inputs are finite; a program needn't handle non-finite values.
Results may differ from the reference program's by a relative error of at most 0.0049.
Values may be sent and summed in bfloat16 or wider, within the bound.
A program may use at most 192 MiB of HBM per device.

```python
import math
import jax
import jax.numpy as jnp
import numpy as np
from jax import lax

ANG = 64
H = 32
Z = 512
TRB = 128
BLK_DEV = 96
IMG_DEV = 4
CAP = 2
POS_DEV = 192
POSITIONS = 49152
BLOCKS = 24576
IT = 16
IMAGE_BLOCKS = 1024
N_SHOT = 64
N_GRP = 4
DEVICES = 256


def draw_offsets(key, part):
    keys = jax.random.split(jax.random.fold_in(key, 11), 3)
    row_scale = jnp.exp(jax.random.uniform(keys[1], (POSITIONS, 1, 1), jnp.float32) * jnp.log(10.0))
    depth_scale = jnp.exp(jax.random.uniform(keys[2], (1, 1, Z), jnp.float32) * jnp.log(10.0))
    place = jnp.arange(POSITIONS, dtype=jnp.float32) / max(POSITIONS - 1, 1)
    base = jnp.clip(jax.random.normal(keys[0], (POSITIONS, H, Z), jnp.float32), -6.0, 6.0)
    ramp = 1.0 + 2.0 * place
    values = 0.1 * base * row_scale * depth_scale * ramp[:, None, None]
    return values.astype(jnp.bfloat16)


def draw_live(key, part):
    cutoff = jax.random.randint(jax.random.fold_in(key, 23), (POSITIONS,), ANG // 4, ANG + 1)
    first = jnp.arange(POSITIONS) % POS_DEV == 0
    cutoff = jnp.where(first, ANG, cutoff)
    return (jnp.arange(ANG)[None, :] < cutoff[:, None]).astype(jnp.int32)


def place_ends(drawn, key, low, top_value):
    spot = [jax.random.randint(jax.random.fold_in(key, axis), (), 0, length) for axis, length in enumerate(drawn.shape)]
    longest = drawn.shape.index(max(drawn.shape))
    next_to = spot[:longest] + [(spot[longest] + 1) % drawn.shape[longest]] + spot[longest + 1:]
    return drawn.at[tuple(spot)].set(low).at[tuple(next_to)].set(top_value)


def deal_out(key, own, number, rows, number_of, top, most, lean):
    order = jax.random.permutation(key, number_of)
    crowded, usual = shares(number_of, rows * top, most, lean, True), shares(number_of, rows * top, most, lean, False)
    places = jnp.arange(number_of)

    def named(lengths, rotation):
        used = int((lengths > 0).sum())
        fixed = max(1, used // 4)
        moved = fixed + (places - fixed + rotation * (used - fixed)) % max(1, number_of - fixed)
        return jnp.zeros((number_of,), jnp.int32).at[order[jnp.where(places < fixed, places, moved)]].set(jnp.asarray(lengths, jnp.int32))

    lengths = jnp.where(number % 4 == 0, named(crowded, number // 4), named(usual, number - number // 4 - 1))
    mixed = jax.random.permutation(jax.random.fold_in(own, 3), number_of)
    giver, receiver = mixed[0:number_of // 2 * 2:2], mixed[1:number_of // 2 * 2:2]
    margin = jnp.minimum(lengths[giver] - 1, most - lengths[receiver]) // 2
    margin = jnp.where((giver == order[0]) | (receiver == order[0]) | (lengths[receiver] == 0), 0, jnp.maximum(margin, 0))
    moved = jax.random.randint(jax.random.fold_in(own, 4), (number_of // 2,), 0, 1 << 20) % (margin + 1)
    lengths = lengths.at[giver].add(-moved).at[receiver].add(moved)
    labels = jnp.searchsorted(jnp.cumsum(lengths), jnp.arange(rows * top), side="right").astype(jnp.int32)
    table = labels.reshape(top, rows).T
    table = table[jax.random.permutation(jax.random.fold_in(own, 1), rows)]
    rotation = jax.random.randint(jax.random.fold_in(own, 2), (rows, 1), 0, top)
    return jnp.take_along_axis(table, (jnp.arange(top)[None, :] + rotation) % top, axis=1)


def shares(number_of, total, reach, lean, full):
    weights = [(1 << 20) // math.isqrt(standing ** lean) + 1 for standing in range(1, number_of + 1)]
    largest = reach if full else min(reach, max(-(-total // number_of), total * weights[0] // sum(weights)))
    least = 1 if total - largest >= number_of - 1 else 0
    counts, spare = [largest] + [least] * (number_of - 1), total - largest - least * (number_of - 1)
    while spare > 0:
        movable = [i for i in range(1, number_of) if counts[i] < largest] or [i for i in range(1, number_of) if counts[i] < reach]
        mass, budget = sum([weights[i] for i in movable]), spare
        for i in movable:
            more = min(reach - counts[i], max(1, budget * weights[i] // mass), spare)
            counts[i] = counts[i] + more
            spare = spare - more
    return np.array(counts)


def noise(rng, shape, width, most, kind=jnp.bfloat16):
    return jnp.clip(width * jax.random.normal(rng, shape, jnp.float32), -most, most).astype(kind)


def setup_inputs(seed: int = 0) -> dict:
    key_list = jax.random.split(jax.random.key(seed), 6)
    offsets = draw_offsets(jax.random.fold_in(key_list[5], 71), 0)
    slant_weights = noise(key_list[1], (ANG, H), H ** -0.5, 1.0)
    live = draw_live(jax.random.fold_in(key_list[5], 71), 0)
    block_tile_keys = jax.random.split(jax.random.fold_in(key_list[3], 1), BLOCKS // BLK_DEV)
    block_tile_turns = jax.random.permutation(jax.random.fold_in(key_list[3], 3), BLOCKS // BLK_DEV)
    block_tile = jax.vmap(lambda own, number: deal_out(jax.random.fold_in(key_list[3], 2), own, number, BLK_DEV, N_SHOT, 1, CAP, 1))(block_tile_keys, block_tile_turns).reshape((BLOCKS, 1))
    image_slot = place_ends(jax.random.randint(key_list[4], (BLOCKS,), 0, IT), jax.random.fold_in(key_list[4], 1), 0, IT - 1).astype(jnp.int32)
    return {"offsets": offsets, "slant_weights": slant_weights, "live": live, "block_tile": block_tile, "image_slot": image_slot}


def reference(offsets, slant_weights, live, block_tile, image_slot):
    tile_rows = IMG_DEV * N_GRP
    weights = slant_weights.astype(jnp.float32)
    shards = (offsets.reshape(DEVICES, POS_DEV, H, Z), live.reshape(DEVICES, POS_DEV, ANG), block_tile.reshape(DEVICES, BLK_DEV), image_slot.reshape(DEVICES, BLK_DEV))

    def advance(state_in, pieces):
        stacked, square_sum, live_count = state_in
        shard_off, shard_live, shard_tile, shard_slot = pieces
        live_mask = shard_live.astype(jnp.float32)
        slanted = jnp.einsum('ah,phz->paz', weights, shard_off.astype(jnp.float32))
        angles = (slanted * live_mask[:, :, None]).astype(jnp.bfloat16)
        widened = angles.astype(jnp.float32)
        square_sum = square_sum + lax.optimization_barrier(jnp.sum(widened * widened, axis=(0, 2)))
        live_count = live_count + lax.optimization_barrier(jnp.sum(live_mask, axis=0))
        targets = (shard_tile.astype(jnp.int32) * tile_rows + shard_slot.astype(jnp.int32)).astype(jnp.int32)
        stacked = stacked.at[targets].add(widened.reshape(BLK_DEV, TRB, Z))
        return ((stacked, square_sum, live_count), None)
    initial = (jnp.zeros((IMAGE_BLOCKS, TRB, Z), jnp.float32), jnp.zeros((ANG,), jnp.float32), jnp.zeros((ANG,), jnp.float32))
    (stacked, square_sum, live_count), unused = lax.scan(advance, initial, shards)
    angle_gain = lax.rsqrt(square_sum / (Z * live_count) + 1e-06)
    trace_gain = jnp.tile(angle_gain, 2)
    return (stacked * trace_gain[None, :, None]).astype(jnp.bfloat16)
```

```python
import functools

import jax
import jax.numpy as jnp
from jax import lax
from jax.experimental import pallas as pl
from jax.experimental.pallas import tpu as pltpu
from jax.sharding import Mesh
from jax.sharding import PartitionSpec as P

SHOT_GRP = ("y", "z", "c", "x")
SLAB = ("x", "y")
ANG = 64
LANES = 128
HALF = 64


def pack_body(low_ref, high_ref, out_ref):
    for quarter in range(4):
        for place in range(2):
            lanes = slice(quarter * LANES, (quarter + 1) * LANES)
            low = low_ref[:, place, :, lanes]
            high = high_ref[:, place, :, lanes]
            out_ref[quarter, 2 * place] = jnp.concatenate(
                [low[..., :HALF], high[..., :HALF]], axis=-1
            )
            out_ref[quarter, 2 * place + 1] = jnp.concatenate(
                [low[..., HALF:], high[..., HALF:]], axis=-1
            )


def packed(blocks):
    count, _, inner, depth = blocks.shape
    pairs, step = count // 2, 8
    return pl.pallas_call(
        pack_body,
        grid=(pairs // step,),
        in_specs=[
            pl.BlockSpec((step, 2, inner, depth), lambda i: (i, 0, 0, 0)),
            pl.BlockSpec((step, 2, inner, depth), lambda i: (i + pairs // step, 0, 0, 0)),
        ],
        out_specs=pl.BlockSpec((4, 4, step, inner, LANES), lambda i: (0, 0, i, 0, 0)),
        out_shape=jax.ShapeDtypeStruct((4, 4, pairs, inner, LANES), jnp.bfloat16),
        cost_estimate=pl.CostEstimate(
            flops=4 * blocks.size, bytes_accessed=4 * blocks.size, transcendentals=0
        ),
    )(blocks, blocks)


def square_body(step, cut_ref, raw_ref, weight_ref, out_ref):
    first = pl.program_id(0)

    @pl.when(first == 0)
    def _():
        out_ref[...] = jnp.zeros_like(out_ref)

    rows = lax.broadcasted_iota(jnp.int32, (ANG, LANES), 0)
    weights = weight_ref[...]
    total = jnp.zeros((ANG, LANES), jnp.float32)
    for i in range(step):
        angles = jnp.dot(weights, raw_ref[i], preferred_element_type=jnp.float32)
        squares = angles * angles
        folded = (squares[:, :128] + squares[:, 128:256]) + (
            squares[:, 256:384] + squares[:, 384:]
        )
        total += jnp.where(rows < cut_ref[first * step + i], folded, 0.0)
    out_ref[...] += total


def square_sums(offsets, weights, cuts):
    count, inner, depth = offsets.shape
    step = 16
    lanes = pl.pallas_call(
        functools.partial(square_body, step),
        grid_spec=pltpu.PrefetchScalarGridSpec(
            num_scalar_prefetch=1,
            grid=(count // step,),
            in_specs=[
                pl.BlockSpec((step, inner, depth), lambda i, cut: (i, 0, 0)),
                pl.BlockSpec((ANG, inner), lambda i, cut: (0, 0)),
            ],
            out_specs=pl.BlockSpec((ANG, LANES), lambda i, cut: (0, 0)),
        ),
        out_shape=jax.ShapeDtypeStruct((ANG, LANES), jnp.float32),
        cost_estimate=pl.CostEstimate(
            flops=2 * ANG * offsets.size, bytes_accessed=2 * offsets.size, transcendentals=0
        ),
    )(cuts, offsets, weights)
    return jnp.sum(lanes, axis=1)


def stack_body(pairs, code_ref, cut_ref, raw_ref, weight_ref, mine_ref, other_ref, acc_ref):
    source = pl.program_id(0)
    half = acc_ref.shape[0] // 2

    @pl.when(source == 0)
    def _():
        def clear(i, carry):
            acc_ref[pl.ds(i * 8, 8)] = jnp.zeros((8, ANG, LANES), jnp.float32)
            return carry

        lax.fori_loop(0, acc_ref.shape[0] // 8, clear, 0)

    rows = lax.broadcasted_iota(jnp.int32, (ANG, LANES), 0)
    weights = weight_ref[...]
    unroll = 8

    def group(i, carry):
        sides, places = [], []
        for u in range(unroll):
            row = raw_ref[0, i * unroll + u]
            zero = jnp.zeros((row.shape[0], HALF), jnp.bfloat16)
            left, right = row[:, :HALF], row[:, HALF:]
            for side, value in ((0, left), (1, right)):
                at = source * 2 * pairs + side * pairs + i * unroll + u
                code = code_ref[at]
                low = jnp.concatenate([value, zero], axis=1)
                high = jnp.concatenate([zero, value], axis=1)
                sides.append(jnp.where(code % 2 == 0, low, high))
                places.append((code // 2, cut_ref[at]))
        angles = jnp.dot(
            weights, jnp.concatenate(sides, axis=1), preferred_element_type=jnp.float32
        )
        for n, (place, cut) in enumerate(places):
            part = angles[:, n * LANES : (n + 1) * LANES]
            acc_ref[place] += jnp.where(rows < cut, part, 0.0)
        return carry

    lax.fori_loop(0, pairs // unroll, group, 0)

    @pl.when(source == pl.num_programs(0) - 1)
    def _():
        def put(i, carry):
            at = pl.ds(i * 8, 8)
            mine_ref[at] = acc_ref[at].astype(mine_ref.dtype)
            other_ref[at] = acc_ref[pl.ds(half + i * 8, 8)].astype(other_ref.dtype)
            return carry

        lax.fori_loop(0, half // 8, put, 0)


def stacked_parts(raw, weights, codes, cuts, places):
    sources, pairs, inner, _ = raw.shape
    shape = (places // 2, ANG, LANES)
    return pl.pallas_call(
        functools.partial(stack_body, pairs),
        grid_spec=pltpu.PrefetchScalarGridSpec(
            num_scalar_prefetch=2,
            grid=(sources,),
            in_specs=[
                pl.BlockSpec((1, pairs, inner, LANES), lambda i, a, b: (i, 0, 0, 0)),
                pl.BlockSpec((ANG, inner), lambda i, a, b: (0, 0)),
            ],
            out_specs=[pl.BlockSpec(shape, lambda i, a, b: (0, 0, 0))] * 2,
            scratch_shapes=[pltpu.VMEM((places, ANG, LANES), jnp.float32)],
        ),
        out_shape=[
            jax.ShapeDtypeStruct(shape, jnp.bfloat16),
            jax.ShapeDtypeStruct(shape, jnp.bfloat16),
        ],
        cost_estimate=pl.CostEstimate(
            flops=4 * ANG * raw.size, bytes_accessed=2 * raw.size, transcendentals=0
        ),
    )(codes, cuts, raw, weights)


def unpack_body(part_ref, out_ref):
    for quarter in range(4):
        for place in range(2):
            for pair in range(2):
                near = part_ref[4 * quarter + 2 * place, pair]
                far = part_ref[4 * quarter + 2 * place + 1, pair]
                at = (
                    slice(place * ANG, (place + 1) * ANG),
                    slice(quarter * LANES, (quarter + 1) * LANES),
                )
                out_ref[2 * pair, at[0], at[1]] = jnp.concatenate(
                    [near[:, :HALF], far[:, :HALF]], axis=1
                )
                out_ref[2 * pair + 1, at[0], at[1]] = jnp.concatenate(
                    [near[:, HALF:], far[:, HALF:]], axis=1
                )


def local(offsets, slant_weights, live, block_tile, image_slot):
    y, z, c = lax.axis_index("y"), lax.axis_index("z"), lax.axis_index("c")
    block_count = block_tile.shape[0]
    positions, inner, depth = offsets.shape
    tile = block_tile[:, 0]
    tile_y, tile_z, tile_c = tile // 16, tile // 2 % 8, tile % 2
    chunk = tile_z
    place = (tile_c ^ c) * 256 + chunk * 32 + image_slot // 4 * 8 + tile_y * 2
    code = (place + image_slot // 2 % 2) * 2 + image_slot % 2
    cuts = jnp.sum(live, axis=1)
    notes = jnp.concatenate([code, cuts])
    notes = lax.all_gather(notes, SLAB, axis=0, tiled=False)
    codes = notes[:, :block_count].reshape(-1)
    own_cuts = notes[:, block_count:].reshape(-1, block_count, 2)
    own_cuts = jnp.where(y // 2 == 0, own_cuts[..., 0], own_cuts[..., 1]).reshape(-1)

    sent = packed(offsets.reshape(block_count, 2, inner, depth))
    raw = lax.all_to_all(
        sent.reshape((16,) + sent.shape[2:]), SLAB, split_axis=0, concat_axis=0, tiled=True
    )
    squares = square_sums(offsets, slant_weights, cuts)
    counts = jnp.sum(live, axis=0).astype(jnp.float32)
    totals = lax.psum(jnp.stack([squares, counts]), SHOT_GRP)
    gain = lax.rsqrt(totals[0] / (depth * totals[1]) + 1e-06)

    mine, other = stacked_parts(raw, slant_weights, codes, own_cuts, 512)
    got = lax.ppermute(other, "c", [(0, 1), (1, 0)])
    both = (mine.astype(jnp.float32) + got.astype(jnp.float32)).astype(jnp.bfloat16)
    summed = lax.psum_scatter(
        both.reshape(8, 32, ANG, LANES), "z", scatter_dimension=0, tiled=False
    )
    scaled = (summed.astype(jnp.float32) * gain[None, :, None]).astype(jnp.bfloat16)
    parts = lax.all_to_all(
        scaled.reshape(16, 2, ANG, LANES), SLAB, split_axis=0, concat_axis=0, tiled=True
    )
    return pl.pallas_call(
        unpack_body,
        out_shape=jax.ShapeDtypeStruct((4, 2 * ANG, depth), jnp.bfloat16),
    )(parts)


def solution(mesh):
    torus = Mesh(mesh.devices.reshape(4, 8, 2, mesh.shape["grp"]), SHOT_GRP)
    return jax.shard_map(
        local,
        mesh=torus,
        in_specs=(P(SHOT_GRP, None, None), P(), P(SHOT_GRP, None), P(SHOT_GRP, None), P(SHOT_GRP)),
        out_specs=P(SHOT_GRP, None, None),
        check_vma=False,
    )
```

```python
import functools

import jax
import jax.numpy as jnp
from jax import lax
from jax.experimental import pallas as pl
from jax.experimental.pallas import tpu as pltpu
from jax.sharding import Mesh
from jax.sharding import PartitionSpec as P

SHOT_GRP = ("y", "z", "c", "x")
SLAB = ("x", "y")
ANG = 64
LANES = 128
HALF = 64


def pack_body(note_ref, low_ref, high_ref, out_ref):
    last = pl.program_id(0) == pl.num_programs(0) - 1

    @pl.when(last)
    def _():
        rows, lanes = note_ref.shape
        for dest in range(16):
            out_ref[dest, 0, :rows] = note_ref[...]

    @pl.when(jnp.logical_not(last))
    def _():
        pack_pairs(low_ref, high_ref, out_ref)


def pack_pairs(low_ref, high_ref, out_ref):
    for quarter in range(4):
        for place in range(2):
            lanes = slice(quarter * LANES, (quarter + 1) * LANES)
            low = low_ref[:, place, :, lanes]
            high = high_ref[:, place, :, lanes]
            out_ref[4 * quarter + 2 * place] = jnp.concatenate(
                [low[..., :HALF], high[..., :HALF]], axis=-1
            )
            out_ref[4 * quarter + 2 * place + 1] = jnp.concatenate(
                [low[..., HALF:], high[..., HALF:]], axis=-1
            )


def packed(blocks, notes):
    count, _, inner, depth = blocks.shape
    pairs, step = count // 2, 8
    steps = pairs // step
    return pl.pallas_call(
        pack_body,
        grid=(steps + 1,),
        in_specs=[
            pl.BlockSpec(notes.shape, lambda i: (0, 0)),
            pl.BlockSpec(
                (step, 2, inner, depth), lambda i: (jnp.minimum(i, steps - 1), 0, 0, 0)
            ),
            pl.BlockSpec(
                (step, 2, inner, depth), lambda i: (jnp.minimum(i, steps - 1) + steps, 0, 0, 0)
            ),
        ],
        out_specs=pl.BlockSpec((16, step, inner, LANES), lambda i: (0, i, 0, 0)),
        out_shape=jax.ShapeDtypeStruct((16, pairs + 1, inner, LANES), jnp.bfloat16),
        cost_estimate=pl.CostEstimate(
            flops=4 * blocks.size, bytes_accessed=4 * blocks.size, transcendentals=0
        ),
    )(notes, blocks, blocks)


def square_body(step, cut_ref, raw_ref, weight_ref, out_ref):
    first = pl.program_id(0)

    @pl.when(first == 0)
    def _():
        out_ref[...] = jnp.zeros_like(out_ref)

    rows = lax.broadcasted_iota(jnp.int32, (ANG, LANES), 0)
    weights = weight_ref[...]
    total = jnp.zeros((ANG, LANES), jnp.float32)
    for i in range(step):
        angles = jnp.dot(weights, raw_ref[i], preferred_element_type=jnp.float32)
        squares = angles * angles
        folded = (squares[:, :128] + squares[:, 128:256]) + (
            squares[:, 256:384] + squares[:, 384:]
        )
        total += jnp.where(rows < cut_ref[first * step + i], folded, 0.0)
    out_ref[...] += total


def square_sums(offsets, weights, cuts):
    count, inner, depth = offsets.shape
    step = 16
    lanes = pl.pallas_call(
        functools.partial(square_body, step),
        grid_spec=pltpu.PrefetchScalarGridSpec(
            num_scalar_prefetch=1,
            grid=(count // step,),
            in_specs=[
                pl.BlockSpec((step, inner, depth), lambda i, cut: (i, 0, 0)),
                pl.BlockSpec((ANG, inner), lambda i, cut: (0, 0)),
            ],
            out_specs=pl.BlockSpec((ANG, LANES), lambda i, cut: (0, 0)),
        ),
        out_shape=jax.ShapeDtypeStruct((ANG, LANES), jnp.float32),
        cost_estimate=pl.CostEstimate(
            flops=2 * ANG * offsets.size, bytes_accessed=2 * offsets.size, transcendentals=0
        ),
    )(cuts, offsets, weights)
    return jnp.sum(lanes, axis=1)


def stack_body(
    pairs, code_ref, cut_ref, raw_ref, weight_ref, gain_ref, mine_ref, other_ref, acc_ref
):
    source = pl.program_id(0)
    half = acc_ref.shape[0] // 2

    @pl.when(source == 0)
    def _():
        def clear(i, carry):
            acc_ref[pl.ds(i * 8, 8)] = jnp.zeros((8, ANG, LANES), jnp.float32)
            return carry

        lax.fori_loop(0, acc_ref.shape[0] // 8, clear, 0)

    rows = lax.broadcasted_iota(jnp.int32, (ANG, LANES), 0)
    weights = weight_ref[...]
    unroll = 8

    def group(i, carry):
        sides, places = [], []
        for u in range(unroll):
            row = raw_ref[0, i * unroll + u]
            zero = jnp.zeros((row.shape[0], HALF), jnp.bfloat16)
            left, right = row[:, :HALF], row[:, HALF:]
            for side, value in ((0, left), (1, right)):
                at = source * 2 * pairs + side * pairs + i * unroll + u
                code = code_ref[at]
                low = jnp.concatenate([value, zero], axis=1)
                high = jnp.concatenate([zero, value], axis=1)
                sides.append(jnp.where(code % 2 == 0, low, high))
                places.append((code // 2, cut_ref[at]))
        angles = jnp.dot(
            weights, jnp.concatenate(sides, axis=1), preferred_element_type=jnp.float32
        )
        for n, (place, cut) in enumerate(places):
            part = angles[:, n * LANES : (n + 1) * LANES]
            acc_ref[place] += jnp.where(rows < cut, part, 0.0)
        return carry

    lax.fori_loop(0, pairs // unroll, group, 0)

    @pl.when(source == pl.num_programs(0) - 1)
    def _():
        def put(i, carry):
            at = pl.ds(i * 8, 8)
            mine_ref[at] = acc_ref[at].astype(mine_ref.dtype)
            other_ref[at] = acc_ref[pl.ds(half + i * 8, 8)].astype(other_ref.dtype)
            return carry

        lax.fori_loop(0, half // 8, put, 0)


def stacked_parts(raw, weights, codes, cuts, places, gain):
    sources, pairs, inner = raw.shape[0], raw.shape[1] - 1, raw.shape[2]
    shape = (places // 2, ANG, LANES)
    return pl.pallas_call(
        functools.partial(stack_body, pairs),
        grid_spec=pltpu.PrefetchScalarGridSpec(
            num_scalar_prefetch=2,
            grid=(sources,),
            in_specs=[
                pl.BlockSpec((1, pairs, inner, LANES), lambda i, a, b: (i, 0, 0, 0)),
                pl.BlockSpec((ANG, inner), lambda i, a, b: (0, 0)),
                pl.BlockSpec(memory_space=pl.ANY),
            ],
            out_specs=[pl.BlockSpec(shape, lambda i, a, b: (0, 0, 0))] * 2,
            scratch_shapes=[pltpu.VMEM((places, ANG, LANES), jnp.float32)],
        ),
        out_shape=[
            jax.ShapeDtypeStruct(shape, jnp.bfloat16),
            jax.ShapeDtypeStruct(shape, jnp.bfloat16),
        ],
        cost_estimate=pl.CostEstimate(
            flops=4 * ANG * raw.size, bytes_accessed=2 * raw.size, transcendentals=0
        ),
    )(codes, cuts, raw, weights, gain)


def total_body(part_ref, out_ref, held, send_sem, recv_sem, sums):
    x, y = lax.axis_index("x"), lax.axis_index("y")
    z, c = lax.axis_index("z"), lax.axis_index("c")
    flat = x * 2 + c

    def near(step):
        peer = lax.rem(flat + step, 8)
        return {"x": peer // 2, "c": lax.rem(peer, 2)}

    stages = (
        [near(step) for step in range(1, 8)],
        [{"y": lax.rem(y + step, 4)} for step in range(1, 4)],
        [{"z": lax.rem(z + step, 8)} for step in range(1, 8)],
    )
    peers = [peer for stage in stages for peer in stage]
    barrier = pltpu.get_barrier_semaphore()
    for peer in peers:
        pl.semaphore_signal(barrier, inc=1, device_id=peer, device_id_type=pl.DeviceIdType.MESH)
    pl.semaphore_wait(barrier, len(peers))

    at = 0
    for number, stage in enumerate(stages):
        source = part_ref if number == 0 else sums.at[number - 1]
        copies = []
        for peer in stage:
            copies.append(
                pltpu.make_async_remote_copy(
                    src_ref=source,
                    dst_ref=held.at[at + len(copies)],
                    send_sem=send_sem.at[at + len(copies)],
                    recv_sem=recv_sem.at[at + len(copies)],
                    device_id=peer,
                    device_id_type=pl.DeviceIdType.MESH,
                )
            )
        for copy in copies:
            copy.start()
        for copy in copies:
            copy.wait()
        total = source[...]
        for n in range(len(copies)):
            total = total + held[at + n]
        at += len(copies)
        if number < 2:
            sums[number] = total
        else:
            out_ref[...] = total


def slice_total(part):
    return pl.pallas_call(
        total_body,
        out_shape=jax.ShapeDtypeStruct(part.shape, jnp.float32),
        in_specs=[pl.BlockSpec(memory_space=pltpu.VMEM)],
        out_specs=pl.BlockSpec(memory_space=pltpu.VMEM),
        scratch_shapes=[
            pltpu.VMEM((17,) + part.shape, jnp.float32),
            pltpu.SemaphoreType.DMA((17,)),
            pltpu.SemaphoreType.DMA((17,)),
            pltpu.VMEM((2,) + part.shape, jnp.float32),
        ],
        compiler_params=pltpu.CompilerParams(collective_id=1, has_side_effects=True),
        cost_estimate=pl.CostEstimate(flops=10**9, bytes_accessed=10**6, transcendentals=0),
    )(part)


UP_ORDER = (2, 3, 0, 1)
DOWN_ORDER = (0, 1, 2, 3)


def reduce_body(
    mine_hbm,
    other_hbm,
    gain_ref,
    out_ref,
    mine,
    got,
    sent,
    came,
    last,
    landed,
    load_sem,
    swap_send,
    swap_recv,
    ring_send,
    ring_recv,
    last_send,
    last_recv,
):
    x, y = lax.axis_index("x"), lax.axis_index("y")
    z, c = lax.axis_index("z"), lax.axis_index("c")
    ring = ({"z": lax.rem(z + 1, 8)}, {"z": lax.rem(z + 7, 8)})
    partner = {"c": 1 - c}
    offsets = [(dx, dy) for dx in range(4) for dy in range(4)][1:]
    spread = [{"x": lax.rem(x + dx, 4), "y": lax.rem(y + dy, 4)} for dx, dy in offsets]

    barrier = pltpu.get_barrier_semaphore()
    peers = [partner, *ring, *spread]
    for peer in peers:
        pl.semaphore_signal(barrier, inc=1, device_id=peer, device_id_type=pl.DeviceIdType.MESH)

    loads, swaps = {}, {}
    for chunk in (4, 3, 5, 2, 6, 1, 7, 0):
        loads[chunk] = pltpu.make_async_copy(
            mine_hbm.at[chunk], mine.at[chunk], load_sem.at[chunk]
        )
        swaps[chunk] = pltpu.make_async_remote_copy(
            src_ref=other_hbm.at[chunk],
            dst_ref=got.at[chunk],
            send_sem=swap_send.at[chunk],
            recv_sem=swap_recv.at[chunk],
            device_id=partner,
            device_id_type=pl.DeviceIdType.MESH,
        )
    pl.semaphore_wait(barrier, len(peers))
    for chunk in swaps:
        swaps[chunk].start()
        loads[chunk].start()

    def own(chunk, part):
        return mine[chunk, part].astype(jnp.float32) + got[chunk, part].astype(jnp.float32)

    copies = {}
    for step in range(4):
        for chunk in ((4,), (3, 5), (2, 6), (1, 7))[step]:
            loads[chunk].wait()
            swaps[chunk].wait()
        for turn in range(4):
            for way, order in enumerate((UP_ORDER, DOWN_ORDER)):
                if step == 0 and turn < 2:
                    continue
                part = order[turn]
                chunk = 4 - step if way == 0 else 4 + step
                value = own(chunk, part)
                before = copies.get((way, step - 1, part))
                if before is not None:
                    before.wait_recv()
                    value = value + came[way, step - 1, part].astype(jnp.float32)
                sent[way, step, part] = value.astype(jnp.bfloat16)
                copy = pltpu.make_async_remote_copy(
                    src_ref=sent.at[way, step, part],
                    dst_ref=came.at[way, step, part],
                    send_sem=ring_send.at[way, step, part],
                    recv_sem=ring_recv.at[way, step, part],
                    device_id=ring[way],
                    device_id_type=pl.DeviceIdType.MESH,
                )
                copy.start()
                copies[way, step, part] = copy
    loads[0].wait()
    swaps[0].wait()
    gain = gain_ref[...]
    for part in (2, 0, 3, 1):
        value = own(0, part)
        for way in range(2):
            copies[way, 3, part].wait_recv()
            value = value + came[way, 3, part].astype(jnp.float32)
        last[part] = (value * gain[None]).astype(jnp.bfloat16)
    ends = []
    for n, ((dx, dy), peer) in enumerate(zip(offsets, spread)):
        copy = pltpu.make_async_remote_copy(
            src_ref=last.at[peer["x"], pl.ds(peer["y"] * 2, 2)],
            dst_ref=landed.at[x * 4 + y],
            send_sem=last_send.at[n],
            recv_sem=last_recv.at[n],
            device_id=peer,
            device_id_type=pl.DeviceIdType.MESH,
        )
        copy.start()
        ends.append(copy)
    landed[x * 4 + y] = last[x, pl.ds(y * 2, 2)]
    for copy in copies.values():
        copy.wait_send()
    for copy in ends:
        copy.wait()
    for quarter in range(4):
        for place in range(2):
            rows = slice(place * ANG, (place + 1) * ANG)
            lanes = slice(quarter * LANES, (quarter + 1) * LANES)
            for pair in range(2):
                near = landed[4 * quarter + 2 * place, pair]
                far = landed[4 * quarter + 2 * place + 1, pair]
                out_ref[2 * pair, rows, lanes] = jnp.concatenate(
                    [near[:, :HALF], far[:, :HALF]], axis=1
                )
                out_ref[2 * pair + 1, rows, lanes] = jnp.concatenate(
                    [near[:, HALF:], far[:, HALF:]], axis=1
                )


def reduced(mine, other, gain, depth):
    piece = (8, ANG, LANES)
    shape = (8, 4) + piece
    dma = pltpu.SemaphoreType.DMA
    return pl.pallas_call(
        reduce_body,
        out_shape=jax.ShapeDtypeStruct((4, 2 * ANG, depth), jnp.bfloat16),
        in_specs=[
            pl.BlockSpec(memory_space=pl.ANY),
            pl.BlockSpec(memory_space=pl.ANY),
            pl.BlockSpec(memory_space=pltpu.VMEM),
        ],
        out_specs=pl.BlockSpec(memory_space=pltpu.VMEM),
        scratch_shapes=[
            pltpu.VMEM(shape, jnp.bfloat16),
            pltpu.VMEM(shape, jnp.bfloat16),
            pltpu.VMEM((2, 4, 4) + piece, jnp.bfloat16),
            pltpu.VMEM((2, 4, 4) + piece, jnp.bfloat16),
            pltpu.VMEM((4,) + piece, jnp.bfloat16),
            pltpu.VMEM((16, 2, ANG, LANES), jnp.bfloat16),
            dma((8,)),
            dma((8,)),
            dma((8,)),
            dma((2, 4, 4)),
            dma((2, 4, 4)),
            dma((15,)),
            dma((15,)),
        ],
        compiler_params=pltpu.CompilerParams(collective_id=2, has_side_effects=True),
        cost_estimate=pl.CostEstimate(flops=10**9, bytes_accessed=10**7, transcendentals=0),
    )(mine.reshape(shape), other.reshape(shape), gain)


def local(offsets, slant_weights, live, block_tile, image_slot):
    y, z, c = lax.axis_index("y"), lax.axis_index("z"), lax.axis_index("c")
    block_count = block_tile.shape[0]
    positions, inner, depth = offsets.shape
    tile = block_tile[:, 0]
    tile_y, tile_z, tile_c = tile // 16, tile // 2 % 8, tile % 2
    chunk = (tile_z - z + 8) % 8
    place = (tile_c ^ c) * 256 + chunk * 32 + image_slot // 4 * 8 + tile_y * 2
    code = (place + image_slot // 2 % 2) * 2 + image_slot % 2
    cuts = jnp.sum(live, axis=1)
    both_cuts = cuts.reshape(block_count, 2)
    notes = jnp.stack([code // 32, code % 32, both_cuts[:, 0], both_cuts[:, 1]])
    notes = jnp.pad(notes.astype(jnp.bfloat16), ((0, 12), (0, LANES - block_count)))

    sent = packed(offsets.reshape(block_count, 2, inner, depth), notes)
    got = lax.all_to_all(sent, SLAB, split_axis=0, concat_axis=0, tiled=True)
    squares = square_sums(offsets, slant_weights, cuts)
    counts = jnp.sum(live, axis=0).astype(jnp.float32)
    part = jnp.pad(jnp.concatenate([squares, counts])[None], ((0, 7), (0, 0)))
    totals = slice_total(part)[0]
    gain = lax.rsqrt(totals[:ANG] / (depth * totals[ANG:]) + 1e-06)
    gain = jnp.broadcast_to(gain[:, None], (ANG, LANES))

    notes_in = got[:, -1, :4, :block_count].astype(jnp.int32)
    codes = (notes_in[:, 0] * 32 + notes_in[:, 1]).reshape(-1)
    own_cuts = jnp.where(y // 2 == 0, notes_in[:, 2], notes_in[:, 3]).reshape(-1)
    mine, other = stacked_parts(got, slant_weights, codes, own_cuts, 512, gain)
    return reduced(mine, other, gain, depth)


def solution(mesh):
    torus = Mesh(mesh.devices.reshape(4, 8, 2, mesh.shape["grp"]), SHOT_GRP)
    return jax.shard_map(
        local,
        mesh=torus,
        in_specs=(P(SHOT_GRP, None, None), P(), P(SHOT_GRP, None), P(SHOT_GRP, None), P(SHOT_GRP)),
        out_specs=P(SHOT_GRP, None, None),
        check_vma=False,
    )
```

```python
import functools

import jax
import jax.numpy as jnp
from jax import lax
from jax.experimental import pallas as pl
from jax.experimental.pallas import tpu as pltpu
from jax.sharding import Mesh
from jax.sharding import PartitionSpec as P

SHOT_GRP = ("y", "z", "c", "x")
ANG = 64
LANES = 128
WAYS = 2
DEPTHS = LANES // WAYS
ROWS = ANG // WAYS
ROUND = 6
TOGETHER = 16
SOURCES = 4
MESH = pl.DeviceIdType.MESH
STEPS = (
    (1, 0), (3, 0), (0, 1), (0, 3), (1, 1), (3, 3), (1, 3), (3, 1),
    (2, 0), (0, 2), (2, 1), (1, 2), (2, 3), (3, 2), (2, 2),
)
EXACT = lax.Precision.HIGHEST


def slab_peers(x, y):
    return [{"x": lax.rem(x + dx, 4), "y": lax.rem(y + dy, 4)} for dx, dy in STEPS]


def greet(peers):
    barrier = pltpu.get_barrier_semaphore()
    for peer in peers:
        pl.semaphore_signal(barrier, inc=1, device_id=peer, device_id_type=MESH)
    pl.semaphore_wait(barrier, len(peers))


def exchange_body(
    cut_ref,
    count_ref,
    note_ref,
    weight_ref,
    offset_hbm,
    raw_hbm,
    notes_hbm,
    sums_ref,
    held,
    sent,
    load_sem,
    send_sem,
    recv_sem,
    own_sem,
    note_send,
    note_recv,
    note_own,
):
    x, y = lax.axis_index("x"), lax.axis_index("y")
    me = x * 4 + y
    peers = slab_peers(x, y)
    groups = held.shape[0] // WAYS
    rounds = groups // ROUND

    def load(turn, way):
        at = pl.ds(way * groups + turn * ROUND, ROUND)
        return pltpu.make_async_copy(offset_hbm.at[at], held.at[at], load_sem.at[turn, way])

    def start_loads(turn, carry):
        for way in range(WAYS):
            load(turn, way).start()
        return carry

    lax.fori_loop(0, rounds, start_loads, 0)
    greet(peers)

    def copy(turn, n):
        at = pl.ds(turn * ROUND, ROUND)
        peer = peers[n]
        return pltpu.make_async_remote_copy(
            src_ref=sent.at[peer["x"] * 4 + peer["y"], at],
            dst_ref=raw_hbm.at[me, at],
            send_sem=send_sem.at[turn, n],
            recv_sem=recv_sem.at[turn, n],
            device_id=peer,
            device_id_type=MESH,
        )

    def keep(turn):
        at = pl.ds(turn * ROUND, ROUND)
        return pltpu.make_async_copy(sent.at[me, at], raw_hbm.at[me, at], own_sem.at[turn])

    notes = []
    for n, peer in enumerate(peers):
        notes.append(
            pltpu.make_async_remote_copy(
                src_ref=note_ref,
                dst_ref=notes_hbm.at[me],
                send_sem=note_send.at[n],
                recv_sem=note_recv.at[n],
                device_id=peer,
                device_id_type=MESH,
            )
        )
    own_note = pltpu.make_async_copy(note_ref, notes_hbm.at[me], note_own)
    own_note.start()
    for note in notes:
        note.start()

    def send(turn, carry):
        for way in range(WAYS):
            load(turn, way).wait()
        at = pl.ds(turn * ROUND, ROUND)
        for quarter in range(4):
            lanes = slice(quarter * LANES, (quarter + 1) * LANES)
            for place in range(2):
                parts = [
                    held[pl.ds(way * groups + turn * ROUND, ROUND), place, :, lanes]
                    for way in range(WAYS)
                ]
                for end in range(2):
                    cut = slice(end * DEPTHS, (end + 1) * DEPTHS)
                    sent[4 * quarter + 2 * place + end, at] = jnp.concatenate(
                        [part[..., cut] for part in parts], axis=-1
                    )
        keep(turn).start()
        for n in range(len(peers)):
            copy(turn, n).start()
        return carry

    lax.fori_loop(0, rounds, send, 0)

    angle = lax.broadcasted_iota(jnp.int32, (ANG, LANES), 0)
    weights = weight_ref[...]

    def square(i, total):
        for place in range(2):
            angles = jnp.dot(weights, held[i, place], preferred_element_type=jnp.float32)
            squares = angles * angles
            folded = (squares[:, :128] + squares[:, 128:256]) + (
                squares[:, 256:384] + squares[:, 384:]
            )
            total = total + jnp.where(angle < cut_ref[2 * i + place], folded, 0.0)
        return total

    total = lax.fori_loop(0, held.shape[0], square, jnp.zeros((ANG, LANES), jnp.float32))
    flat = lax.dot_general(
        jnp.ones((8, LANES), jnp.float32),
        total,
        (((1,), (1,)), ((), ())),
        precision=EXACT,
        preferred_element_type=jnp.float32,
    )
    sums_ref[...] = jnp.concatenate([flat, count_ref[...]], axis=1)

    own_note.wait()
    for note in notes:
        note.wait()

    def finish(turn, carry):
        keep(turn).wait()
        for n in range(len(peers)):
            copy(turn, n).wait()
        return carry

    lax.fori_loop(0, rounds, finish, 0)


def exchanged(blocks, weights, notes, cuts, counts):
    count, _, inner, depth = blocks.shape
    groups = count // WAYS
    rounds = groups // ROUND
    dma = pltpu.SemaphoreType.DMA
    vmem = pl.BlockSpec(memory_space=pltpu.VMEM)
    return pl.pallas_call(
        exchange_body,
        out_shape=[
            jax.ShapeDtypeStruct((16, groups, inner, LANES), jnp.bfloat16),
            jax.ShapeDtypeStruct((16,) + notes.shape, jnp.bfloat16),
            jax.ShapeDtypeStruct((8, LANES), jnp.float32),
        ],
        in_specs=[
            pl.BlockSpec(memory_space=pltpu.SMEM),
            vmem,
            vmem,
            vmem,
            pl.BlockSpec(memory_space=pl.ANY),
        ],
        out_specs=[
            pl.BlockSpec(memory_space=pl.ANY),
            pl.BlockSpec(memory_space=pl.ANY),
            vmem,
        ],
        scratch_shapes=[
            pltpu.VMEM(blocks.shape, jnp.bfloat16),
            pltpu.VMEM((16, groups, inner, LANES), jnp.bfloat16),
            dma((rounds, WAYS)),
            dma((rounds, 15)),
            dma((rounds, 15)),
            dma((rounds,)),
            dma((15,)),
            dma((15,)),
            dma(()),
        ],
        compiler_params=pltpu.CompilerParams(collective_id=1, has_side_effects=True),
        cost_estimate=pl.CostEstimate(flops=10**9, bytes_accessed=10**7, transcendentals=0),
    )(cuts, counts, notes, weights, blocks)


def stack_body(
    groups, code_ref, cut_ref, raw_ref, weight_ref, mine_ref, other_ref, acc_ref, even_ref, odd_ref
):
    part = pl.program_id(0)
    half = acc_ref.shape[0] // 2
    sources, _, inner, _ = raw_ref.shape
    per_source = groups // TOGETHER
    turns = sources * per_source

    @pl.when(part == 0)
    def _():
        def clear(i, carry):
            acc_ref[pl.ds(i * 16, 16)] = jnp.zeros((16, ROWS, LANES), jnp.float32)
            return carry

        lax.fori_loop(0, acc_ref.shape[0] // 16, clear, 0)

    angle = lax.broadcasted_iota(jnp.int32, (ROWS, LANES), 0) + ROWS * (
        lax.broadcasted_iota(jnp.int32, (ROWS, LANES), 1) // DEPTHS
    )
    lane_group = lax.broadcasted_iota(jnp.int32, (inner, LANES), 1) // DEPTHS
    weights = weight_ref[...]

    def slant(turn, into_ref):
        source, first = turn // per_source, turn % per_source * TOGETHER
        tiles = []
        for u in range(TOGETHER):
            row = raw_ref[source, first + u]
            turned = [row] + [
                jnp.concatenate([row[:, t * DEPTHS :], row[:, : t * DEPTHS]], axis=1)
                for t in range(1, WAYS)
            ]
            for way in range(WAYS):
                tiles.append(
                    jnp.concatenate(
                        [
                            jnp.where(
                                lane_group == group, turned[(way - group) % WAYS], 0
                            ).astype(jnp.bfloat16)
                            for group in range(WAYS)
                        ],
                        axis=0,
                    )
                )
        angles = jnp.dot(
            weights, jnp.concatenate(tiles, axis=1), preferred_element_type=jnp.float32
        )
        for n in range(len(tiles)):
            into_ref[n] = angles[:, n * LANES : (n + 1) * LANES]

    def stack(turn, from_ref):
        source, first = turn // per_source, turn % per_source * TOGETHER
        base = (part * sources + source) * WAYS * groups + first
        places, parts = [], []
        for u in range(TOGETHER):
            for way in range(WAYS):
                at = base + way * groups + u
                places.append(code_ref[at])
                parts.append(jnp.where(angle < cut_ref[at], from_ref[u * WAYS + way], 0.0))
        for n in range(0, len(parts), 2):
            one, two = places[n], places[n + 1]
            first_sum, second_sum = acc_ref[one], acc_ref[two]
            again = jnp.where(one == two, parts[n], 0.0)
            acc_ref[one] = first_sum + parts[n]
            acc_ref[two] = (second_sum + parts[n + 1]) + again

    slant(0, even_ref)

    def step(i, carry):
        slant(2 * i + 1, odd_ref)
        stack(2 * i, even_ref)
        slant(jnp.minimum(2 * i + 2, turns - 1), even_ref)
        stack(2 * i + 1, odd_ref)
        return carry

    lax.fori_loop(0, turns // 2, step, 0)

    @pl.when(part == pl.num_programs(0) - 1)
    def _():
        def put(i, carry):
            at = pl.ds(i * 16, 16)
            mine_ref[at] = acc_ref[at].astype(mine_ref.dtype)
            other_ref[at] = acc_ref[pl.ds(half + i * 16, 16)].astype(other_ref.dtype)
            return carry

        lax.fori_loop(0, half // 16, put, 0)


def stacked_parts(raw, weights, codes, cuts, places):
    sources, groups, inner, _ = raw.shape
    shape = (places // 2, ROWS, LANES)
    buffer = pltpu.VMEM((TOGETHER * WAYS, ROWS, LANES), jnp.float32)
    return pl.pallas_call(
        functools.partial(stack_body, groups),
        grid_spec=pltpu.PrefetchScalarGridSpec(
            num_scalar_prefetch=2,
            grid=(sources // SOURCES,),
            in_specs=[
                pl.BlockSpec((SOURCES, groups, inner, LANES), lambda i, a, b: (i, 0, 0, 0)),
                pl.BlockSpec((ROWS, WAYS * inner), lambda i, a, b: (0, 0)),
            ],
            out_specs=[pl.BlockSpec(shape, lambda i, a, b: (0, 0, 0))] * 2,
            scratch_shapes=[pltpu.VMEM((places, ROWS, LANES), jnp.float32), buffer, buffer],
        ),
        out_shape=[jax.ShapeDtypeStruct(shape, jnp.bfloat16)] * 2,
        cost_estimate=pl.CostEstimate(
            flops=4 * ANG * raw.size, bytes_accessed=2 * raw.size, transcendentals=0
        ),
    )(codes, cuts, raw, weights)


UP_ORDER = (2, 3, 0, 1)
DOWN_ORDER = (0, 1, 2, 3)


def reduce_body(
    sums_ref,
    mine_hbm,
    other_hbm,
    out_ref,
    mine,
    got,
    sent,
    came,
    last,
    landed,
    sums,
    sums_in,
    load_sem,
    swap_send,
    swap_recv,
    ring_send,
    ring_recv,
    last_send,
    last_recv,
    sums_send,
    sums_recv,
):
    x, y = lax.axis_index("x"), lax.axis_index("y")
    z, c = lax.axis_index("z"), lax.axis_index("c")
    ring = ({"z": lax.rem(z + 1, 8)}, {"z": lax.rem(z + 7, 8)})
    partner = {"c": 1 - c}
    spread = slab_peers(x, y)
    column = [{"z": lax.rem(z + step, 8)} for step in range(1, 8)]
    depth = out_ref.shape[-1]

    loads, swaps = {}, {}
    for chunk in (4, 3, 5, 2, 6, 1, 7, 0):
        loads[chunk] = pltpu.make_async_copy(
            mine_hbm.at[chunk], mine.at[chunk], load_sem.at[chunk]
        )
        loads[chunk].start()
        swaps[chunk] = pltpu.make_async_remote_copy(
            src_ref=other_hbm.at[chunk],
            dst_ref=got.at[chunk],
            send_sem=swap_send.at[chunk],
            recv_sem=swap_recv.at[chunk],
            device_id=partner,
            device_id_type=MESH,
        )
    greet([partner, *column, *spread])
    for chunk in swaps:
        swaps[chunk].start()

    sum_base = (0, 1, 16)
    sum_peers = ([partner], spread, column)

    def sum_copies(stage):
        source = sums_ref if stage == 0 else sums.at[stage - 1]
        return [
            pltpu.make_async_remote_copy(
                src_ref=source,
                dst_ref=sums_in.at[sum_base[stage] + n],
                send_sem=sums_send.at[sum_base[stage] + n],
                recv_sem=sums_recv.at[sum_base[stage] + n],
                device_id=peer,
                device_id_type=MESH,
            )
            for n, peer in enumerate(sum_peers[stage])
        ]

    def sum_wait(stage, flying):
        for copy in flying:
            copy.wait()
        total = sums_ref[...] if stage == 0 else sums[stage - 1]
        for n in range(len(flying)):
            total = total + sums_in[sum_base[stage] + n]
        sums[stage] = total

    def own(chunk, part):
        return mine[chunk, part].astype(jnp.float32) + got[chunk, part].astype(jnp.float32)

    flying = sum_copies(0)
    for copy in flying:
        copy.start()
    copies = {}
    for step in range(4):
        for chunk in ((4,), (3, 5), (2, 6), (1, 7))[step]:
            loads[chunk].wait()
            swaps[chunk].wait()
        for turn in range(4):
            for way, order in enumerate((UP_ORDER, DOWN_ORDER)):
                if step == 0 and turn < 2:
                    continue
                part = order[turn]
                chunk = 4 - step if way == 0 else 4 + step
                value = own(chunk, part)
                before = copies.get((way, step - 1, part))
                if before is not None:
                    before.wait_recv()
                    value = value + came[way, step - 1, part].astype(jnp.float32)
                sent[way, step, part] = value.astype(jnp.bfloat16)
                copy = pltpu.make_async_remote_copy(
                    src_ref=sent.at[way, step, part],
                    dst_ref=came.at[way, step, part],
                    send_sem=ring_send.at[way, step, part],
                    recv_sem=ring_recv.at[way, step, part],
                    device_id=ring[way],
                    device_id_type=MESH,
                )
                copy.start()
                copies[way, step, part] = copy
        if step < 2:
            sum_wait(step, flying)
            flying = sum_copies(step + 1)
            for copy in flying:
                copy.start()
    loads[0].wait()
    swaps[0].wait()
    sum_wait(2, flying)
    totals = sums[2]
    gain = lax.rsqrt(totals[:, :ANG] / (depth * totals[:, ANG:]) + 1e-06)
    angle = lax.broadcasted_iota(jnp.int32, (ROWS, ANG), 1)
    row = lax.broadcasted_iota(jnp.int32, (ROWS, ANG), 0)
    picked = jnp.where(angle % ROWS == row, jnp.broadcast_to(gain[:1], (ROWS, ANG)), 0.0)
    angle = lax.broadcasted_iota(jnp.int32, (ANG, LANES), 0)
    lane = lax.broadcasted_iota(jnp.int32, (ANG, LANES), 1)
    chosen = jnp.where(angle // ROWS == lane // DEPTHS, 1.0, 0.0)
    gain = jnp.dot(picked, chosen, precision=EXACT, preferred_element_type=jnp.float32)
    for part in (2, 0, 3, 1):
        value = own(0, part)
        for way in range(2):
            copies[way, 3, part].wait_recv()
            value = value + came[way, 3, part].astype(jnp.float32)
        last[part] = (value * gain[None]).astype(jnp.bfloat16)
    ends = []
    for n, peer in enumerate(spread):
        copy = pltpu.make_async_remote_copy(
            src_ref=last.at[peer["x"], pl.ds(peer["y"] * 4, 4)],
            dst_ref=landed.at[x * 4 + y],
            send_sem=last_send.at[n],
            recv_sem=last_recv.at[n],
            device_id=peer,
            device_id_type=MESH,
        )
        copy.start()
        ends.append(copy)
    landed[x * 4 + y] = last[x, pl.ds(y * 4, 4)]
    for copy in copies.values():
        copy.wait_send()
    for copy in ends:
        copy.wait()
    for slot in range(4):
        for quarter in range(4):
            lanes = slice(quarter * LANES, (quarter + 1) * LANES)
            for place in range(2):
                ends_in = [landed[4 * quarter + 2 * place + end, slot] for end in range(2)]
                for group in range(WAYS):
                    at = place * ANG + group * ROWS
                    cut = slice(group * DEPTHS, (group + 1) * DEPTHS)
                    out_ref[slot, at : at + ROWS, lanes] = jnp.concatenate(
                        [part[:, cut] for part in ends_in], axis=1
                    )


def reduced(sums, mine, other, depth):
    piece = (mine.shape[0] // 32, ROWS, LANES)
    shape = (8, 4) + piece
    dma = pltpu.SemaphoreType.DMA
    vmem = pl.BlockSpec(memory_space=pltpu.VMEM)
    return pl.pallas_call(
        reduce_body,
        out_shape=jax.ShapeDtypeStruct((4, 2 * ANG, depth), jnp.bfloat16),
        in_specs=[
            vmem,
            pl.BlockSpec(memory_space=pl.ANY),
            pl.BlockSpec(memory_space=pl.ANY),
        ],
        out_specs=vmem,
        scratch_shapes=[
            pltpu.VMEM(shape, jnp.bfloat16),
            pltpu.VMEM(shape, jnp.bfloat16),
            pltpu.VMEM((2, 4, 4) + piece, jnp.bfloat16),
            pltpu.VMEM((2, 4, 4) + piece, jnp.bfloat16),
            pltpu.VMEM((4,) + piece, jnp.bfloat16),
            pltpu.VMEM((16, 4, ROWS, LANES), jnp.bfloat16),
            pltpu.VMEM((3,) + sums.shape, jnp.float32),
            pltpu.VMEM((23,) + sums.shape, jnp.float32),
            dma((8,)),
            dma((8,)),
            dma((8,)),
            dma((2, 4, 4)),
            dma((2, 4, 4)),
            dma((15,)),
            dma((15,)),
            dma((23,)),
            dma((23,)),
        ],
        compiler_params=pltpu.CompilerParams(collective_id=2, has_side_effects=True),
        cost_estimate=pl.CostEstimate(flops=10**9, bytes_accessed=10**7, transcendentals=0),
    )(sums, mine.reshape(shape), other.reshape(shape))


def local(offsets, slant_weights, live, block_tile, image_slot):
    y, z, c = lax.axis_index("y"), lax.axis_index("z"), lax.axis_index("c")
    block_count = block_tile.shape[0]
    positions, inner, depth = offsets.shape
    tile = block_tile[:, 0]
    tile_y, tile_z, tile_c = tile // 16, tile // 2 % 8, tile % 2
    chunk = (tile_z - z + 8) % 8
    code = (tile_c ^ c) * 512 + chunk * 64 + image_slot // 4 * 16 + tile_y * 4 + image_slot % 4
    cuts = jnp.sum(live, axis=1)
    both_cuts = cuts.reshape(block_count, 2)
    notes = jnp.stack([code // 32, code % 32, both_cuts[:, 0], both_cuts[:, 1]])
    notes = jnp.pad(notes.astype(jnp.bfloat16), ((0, 12), (0, LANES - block_count)))
    counts = jnp.broadcast_to(jnp.sum(live, axis=0).astype(jnp.float32)[None], (8, ANG))

    raw, notes_in, sums = exchanged(
        offsets.reshape(block_count, 2, inner, depth), slant_weights, notes, cuts, counts
    )
    notes_in = notes_in[:, :4, :block_count].astype(jnp.int32)
    codes = (notes_in[:, 0] * 32 + notes_in[:, 1]).reshape(-1)
    own_cuts = jnp.where(y // 2 == 0, notes_in[:, 2], notes_in[:, 3]).reshape(-1)
    side_by_side = slant_weights.reshape(WAYS, ROWS, inner).transpose(1, 0, 2)
    mine, other = stacked_parts(
        raw, side_by_side.reshape(ROWS, WAYS * inner), codes, own_cuts, 1024
    )
    return reduced(sums, mine, other, depth)


def solution(mesh):
    torus = Mesh(mesh.devices.reshape(4, 8, 2, mesh.shape["grp"]), SHOT_GRP)
    return jax.shard_map(
        local,
        mesh=torus,
        in_specs=(P(SHOT_GRP, None, None), P(), P(SHOT_GRP, None), P(SHOT_GRP, None), P(SHOT_GRP)),
        out_specs=P(SHOT_GRP, None, None),
        check_vma=False,
    )
```

```python
import functools

import jax
import jax.numpy as jnp
from jax import lax
from jax.experimental import pallas as pl
from jax.experimental.pallas import tpu as pltpu
from jax.sharding import Mesh
from jax.sharding import PartitionSpec as P

SHOT_GRP = ("y", "z", "c", "x")
ANG = 64
LANES = 128
WAYS = 2
DEPTHS = LANES // WAYS
ROWS = ANG // WAYS
ROUND = 6
SLOTS = 16
PLACES = 1024
TILE = 256
MESH = pl.DeviceIdType.MESH
STEPS = (
    (1, 0), (3, 0), (0, 1), (0, 3), (1, 1), (3, 3), (1, 3), (3, 1),
    (2, 0), (0, 2), (2, 1), (1, 2), (2, 3), (3, 2), (2, 2),
)
UP_ORDER = (2, 3, 0, 1)
DOWN_ORDER = (0, 1, 2, 3)
EXACT = lax.Precision.HIGHEST


def exact_dot(a, b, dims):
    return lax.dot_general(
        a, b, (dims, ((), ())), precision=EXACT, preferred_element_type=jnp.float32
    )


def body(
    cut_ref,
    live_ref,
    tile_ref,
    slot_ref,
    weight_ref,
    offset_hbm,
    out_ref,
    held,
    sent,
    raw,
    acc,
    angles,
    chosen,
    cut_rows,
    even_side,
    odd_side,
    note,
    notes,
    note_sums,
    other,
    got,
    ring_out,
    ring_in,
    turned,
    last,
    landed,
    sums,
    sums_in,
    load_sem,
    send_sem,
    recv_sem,
    note_send,
    note_recv,
    swap_send,
    swap_recv,
    ring_send,
    ring_recv,
    last_send,
    last_recv,
    sums_send,
    sums_recv,
):
    x, y = lax.axis_index("x"), lax.axis_index("y")
    z, c = lax.axis_index("z"), lax.axis_index("c")
    me = x * 4 + y
    spread = [{"x": lax.rem(x + dx, 4), "y": lax.rem(y + dy, 4)} for dx, dy in STEPS]
    column = [{"z": lax.rem(z + step, 8)} for step in range(1, 8)]
    ring = (column[0], column[-1])
    partner = {"c": 1 - c}
    groups = held.shape[0] // WAYS
    rounds = groups // ROUND
    block_count, positions = tile_ref.shape[1], live_ref.shape[1]
    depth = held.shape[-1]

    def remote(source, target, send, recv, peer):
        return pltpu.make_async_remote_copy(
            src_ref=source,
            dst_ref=target,
            send_sem=send,
            recv_sem=recv,
            device_id=peer,
            device_id_type=MESH,
        )

    def load(turn, way):
        at = pl.ds(way * groups + turn * ROUND, ROUND)
        return pltpu.make_async_copy(offset_hbm.at[at], held.at[at], load_sem.at[turn, way])

    def start_loads(turn, carry):
        for way in range(WAYS):
            load(turn, way).start()
        return carry

    lax.fori_loop(0, rounds, start_loads, 0)

    tile, slot = tile_ref[...], slot_ref[...]
    code = ((tile & 1) ^ c) * 512 + ((((tile >> 1) & 7) - z + 8) & 7) * 64
    code = code + (slot >> 2) * 16 + (tile >> 4) * 4 + (slot & 3) + 1
    live = live_ref[...].astype(jnp.float32)
    position = lax.broadcasted_iota(jnp.int32, (positions, block_count), 0)
    block = lax.broadcasted_iota(jnp.int32, (positions, block_count), 1)
    live_cuts = jnp.broadcast_to(jnp.sum(live, axis=0, keepdims=True), (8, positions))
    values = [(code >> 5).astype(jnp.float32), (code & 31).astype(jnp.float32)]
    for place in range(2):
        pick = jnp.where(position == 2 * block + place, 1.0, 0.0)
        values.append(exact_dot(live_cuts, pick, ((1,), (0,)))[:1])
    turn_of = lax.broadcasted_iota(jnp.int32, (rounds, block_count), 1) % groups // ROUND
    own_turn = lax.broadcasted_iota(jnp.int32, (rounds, block_count), 0)
    spot = lax.broadcasted_iota(jnp.int32, (block_count, LANES), 0)
    lane = lax.broadcasted_iota(jnp.int32, (block_count, LANES), 1)
    spot = spot // groups * ROUND + spot % groups % ROUND + (me & 7) * SLOTS
    move = jnp.where(spot == lane, 1.0, 0.0)
    rows = [
        exact_dot(
            jnp.where(
                turn_of == own_turn, jnp.broadcast_to(value, (rounds, block_count)), 0.0
            ),
            move,
            ((1,), (0,)),
        )
        for value in values
    ]
    own_note = jnp.concatenate(rows, axis=0).astype(jnp.bfloat16)
    note[...] = own_note
    notes[me] = own_note
    weights = jnp.transpose(weight_ref[...].astype(jnp.float32)).astype(jnp.bfloat16)

    peers = [partner, *column, *spread]
    barrier = pltpu.get_barrier_semaphore()
    for peer in peers:
        pl.semaphore_signal(barrier, inc=1, device_id=peer, device_id_type=MESH)
    pl.semaphore_wait(barrier, len(peers))

    note_copies = [
        remote(note, notes.at[me], note_send.at[n], note_recv.at[n], peer)
        for n, peer in enumerate(spread)
    ]
    for copy in note_copies:
        copy.start()

    def copy(turn, n):
        at = pl.ds(turn * ROUND, ROUND)
        peer = spread[n]
        return remote(
            sent.at[peer["x"] * 4 + peer["y"], at],
            raw.at[me, at],
            send_sem.at[turn, n],
            recv_sem.at[turn, n],
            peer,
        )

    def send(turn, carry):
        for way in range(WAYS):
            load(turn, way).wait()
        at = pl.ds(turn * ROUND, ROUND)
        for quarter in range(4):
            lanes = slice(quarter * LANES, (quarter + 1) * LANES)
            for place in range(2):
                parts = [
                    held[pl.ds(way * groups + turn * ROUND, ROUND), place, :, lanes]
                    for way in range(WAYS)
                ]
                for end in range(2):
                    low = end * DEPTHS
                    sent[4 * quarter + 2 * place + end, at] = jnp.concatenate(
                        [part[..., low : low + DEPTHS] for part in parts], axis=-1
                    )
        for n in range(len(spread)):
            copy(turn, n).start()
        raw[me, at] = sent[me, at]
        return carry

    lax.fori_loop(0, rounds, send, 0)

    angle = lax.broadcasted_iota(jnp.int32, (ANG, LANES), 0)

    def square(i, total):
        for place in range(2):
            part = jnp.dot(weights, held[i, place], preferred_element_type=jnp.float32)
            squares = part * part
            folded = (squares[:, :128] + squares[:, 128:256]) + (
                squares[:, 256:384] + squares[:, 384:]
            )
            total = total + jnp.where(angle < cut_ref[2 * i + place], folded, 0.0)
        return total

    total = lax.fori_loop(0, held.shape[0], square, jnp.zeros((ANG, LANES), jnp.float32))
    along = ((1,), (1,))
    sums[0] = jnp.concatenate(
        [
            exact_dot(jnp.ones((8, LANES), jnp.float32), total, along),
            exact_dot(jnp.ones((8, positions), jnp.float32), live, along),
        ],
        axis=1,
    )
    sum_base = (0, 1, 16)
    sum_peers = ([partner], spread, column)

    def sum_start(stage):
        flying = []
        for n, peer in enumerate(sum_peers[stage], sum_base[stage]):
            flying.append(
                remote(sums.at[stage], sums_in.at[n], sums_send.at[n], sums_recv.at[n], peer)
            )
            flying[-1].start()
        return flying

    def sum_wait(stage, flying):
        for piece in flying:
            piece.wait()
        total = sums[stage]
        for n in range(len(flying)):
            total = total + sums_in[sum_base[stage] + n]
        sums[stage + 1] = total

    flying = sum_start(0)

    def clear(i, carry):
        acc[:, pl.ds(i * 8, 8)] = jnp.zeros((ROWS, 8, LANES), jnp.float32)
        return carry

    lax.fori_loop(0, PLACES // 8, clear, 0)

    def clear_angles(i, carry):
        angles[pl.ds(i * SLOTS * ROWS, SLOTS * ROWS)] = jnp.zeros(
            (SLOTS * ROWS, LANES), jnp.float32
        )
        return carry

    lax.fori_loop(0, 16, clear_angles, 0)
    sum_wait(0, flying)
    flying = sum_start(1)
    for piece in note_copies:
        piece.wait()
    for half in range(2):
        total = notes[half * 8].astype(jnp.float32)
        for n in range(1, 8):
            total = total + notes[half * 8 + n].astype(jnp.float32)
        high, low = total[:rounds], total[rounds : 2 * rounds]
        near, far = total[2 * rounds : 3 * rounds], total[3 * rounds :]
        note_sums[0, :, half * LANES : (half + 1) * LANES] = high * 32.0 + low
        note_sums[1, :, half * LANES : (half + 1) * LANES] = jnp.where(y < 2, near, far)

    low_lanes = lax.broadcasted_iota(jnp.int32, (ROWS, LANES), 1) < DEPTHS
    lane_group = lax.broadcasted_iota(jnp.int32, (TILE, LANES), 1) // DEPTHS
    together = 4

    def stack(turn, carry):
        for n in range(len(spread)):
            copy(turn, n).wait()

        def slant(i, inner_carry):
            rows = []
            for u in range(together):
                for n in range(ROUND):
                    rows.append(raw[i * together + u, turn * ROUND + n])
            part = jnp.dot(
                weights, jnp.concatenate(rows, axis=1), preferred_element_type=jnp.float32
            )
            for u in range(together):
                for n in range(ROUND):
                    at = (u * ROUND + n) * LANES
                    row = part[:, at : at + LANES]
                    swapped = pltpu.roll(row, DEPTHS, 1)
                    first = jnp.where(low_lanes, row[:ROWS], swapped[ROWS:])
                    second = jnp.where(low_lanes, swapped[:ROWS], row[ROWS:])
                    base = ((i * together + u) * SLOTS + n) * ROWS
                    angles[pl.ds(base, ROWS)] = first
                    angles[pl.ds(base + ROUND * ROWS, ROWS)] = second
            return inner_carry

        lax.fori_loop(0, 16 // together, slant, 0)

        codes = note_sums[0, pl.ds(turn, 1), :]

        def choose(i, inner_carry):
            place = lax.broadcasted_iota(jnp.int32, (64, 16 * SLOTS), 0) + (i * 64 + 1)
            same = place.astype(jnp.float32) == codes
            chosen[pl.ds(i * 64, 64)] = jnp.where(same, 1.0, 0.0).astype(jnp.bfloat16)
            return inner_carry

        lax.fori_loop(0, PLACES // 64, choose, 0)
        mark = lax.broadcasted_iota(jnp.int32, (rounds, LANES), 0) == turn
        cut = exact_dot(
            note_sums[1], jnp.where(mark, 1.0, 0.0).astype(jnp.float32), ((0,), (0,))
        )
        cut_rows[...] = cut - (lane_group * ROWS).astype(jnp.float32)

        def gather(pair, side):
            for n in range(2):
                r = 2 * pair + n
                part = angles[pl.ds(r, 16 * SLOTS, stride=ROWS), :]
                keep = cut_rows[...] > lax.convert_element_type(r, jnp.float32)
                side[:, n * LANES : (n + 1) * LANES] = jnp.where(keep, part, 0.0).astype(
                    jnp.bfloat16
                )

        def product(pair, side):
            value = side[...]
            for n in range(PLACES // TILE):
                at = pl.ds(n * TILE, TILE)
                part = jnp.dot(chosen[at], value, preferred_element_type=jnp.float32)
                acc[2 * pair, at] += part[:, :LANES]
                acc[2 * pair + 1, at] += part[:, LANES:]

        gather(0, even_side)

        def add(i, inner_carry):
            gather(2 * i + 1, odd_side)
            product(2 * i, even_side)
            gather(jnp.minimum(2 * i + 2, ROWS // 2 - 1), even_side)
            product(2 * i + 1, odd_side)
            return inner_carry

        lax.fori_loop(0, ROWS // 4, add, 0)
        return carry

    lax.fori_loop(0, rounds, stack, 0)

    swaps = {}
    for chunk in (4, 3, 5, 2, 6, 1, 7, 0):
        other[chunk] = acc[:, 512 + chunk * 64 : 512 + (chunk + 1) * 64].astype(jnp.bfloat16)
        swaps[chunk] = remote(
            other.at[chunk], got.at[chunk], swap_send.at[chunk], swap_recv.at[chunk], partner
        )
        swaps[chunk].start()
    sum_wait(1, flying)
    flying = sum_start(2)

    def own(chunk, part):
        at = chunk * 64 + part * 16
        return acc[:, at : at + 16] + got[chunk, :, part * 16 : (part + 1) * 16].astype(
            jnp.float32
        )

    copies = {}
    for step in range(4):
        for chunk in ((4,), (3, 5), (2, 6), (1, 7))[step]:
            swaps[chunk].wait()
        for number in range(4):
            for way, order in enumerate((UP_ORDER, DOWN_ORDER)):
                if step == 0 and number < 2:
                    continue
                part = order[number]
                value = own(4 - step if way == 0 else 4 + step, part)
                before = copies.get((way, step - 1, part))
                if before is not None:
                    before.wait_recv()
                    value = value + ring_in[way, step - 1, part].astype(jnp.float32)
                ring_out[way, step, part] = value.astype(jnp.bfloat16)
                piece = remote(
                    ring_out.at[way, step, part],
                    ring_in.at[way, step, part],
                    ring_send.at[way, step, part],
                    ring_recv.at[way, step, part],
                    ring[way],
                )
                piece.start()
                copies[way, step, part] = piece
    swaps[0].wait()
    sum_wait(2, flying)
    totals = sums[3]
    gain = lax.rsqrt(totals[:, :ANG] / (depth * totals[:, ANG:]) + 1e-06)
    angle = lax.broadcasted_iota(jnp.int32, (ROWS, ANG), 1)
    row = lax.broadcasted_iota(jnp.int32, (ROWS, ANG), 0)
    picked = jnp.where(angle % ROWS == row, jnp.broadcast_to(gain[:1], (ROWS, ANG)), 0.0)
    angle = lax.broadcasted_iota(jnp.int32, (ANG, LANES), 0)
    lane = lax.broadcasted_iota(jnp.int32, (ANG, LANES), 1)
    gain = exact_dot(
        picked, jnp.where(angle // ROWS == lane // DEPTHS, 1.0, 0.0), ((1,), (0,))
    )
    for part in (2, 0, 3, 1):
        value = own(0, part)
        for way in range(2):
            copies[way, 3, part].wait_recv()
            value = value + ring_in[way, 3, part].astype(jnp.float32)
        turned[...] = value.reshape(ROWS * 16, LANES)
        for n in range(16):
            rows = turned[pl.ds(n, ROWS, stride=16), :]
            last[part, n] = (rows * gain).astype(jnp.bfloat16)
    ends = []
    for n, peer in enumerate(spread):
        piece = remote(
            last.at[peer["x"], pl.ds(peer["y"] * 4, 4)],
            landed.at[me],
            last_send.at[n],
            last_recv.at[n],
            peer,
        )
        piece.start()
        ends.append(piece)
    landed[me] = last[x, pl.ds(y * 4, 4)]
    for piece in copies.values():
        piece.wait_send()
    for piece in ends:
        piece.wait()
    for slot in range(4):
        for quarter in range(4):
            lanes = slice(quarter * LANES, (quarter + 1) * LANES)
            for place in range(2):
                parts = [landed[4 * quarter + 2 * place + end, slot] for end in range(2)]
                for group in range(WAYS):
                    at = place * ANG + group * ROWS
                    cut = slice(group * DEPTHS, (group + 1) * DEPTHS)
                    out_ref[slot, at : at + ROWS, lanes] = jnp.concatenate(
                        [part[:, cut] for part in parts], axis=1
                    )


def local(offsets, slant_weights, live, block_tile, image_slot):
    block_count = block_tile.shape[0]
    positions, inner, depth = offsets.shape
    groups = block_count // WAYS
    rounds = groups // ROUND
    dma = pltpu.SemaphoreType.DMA
    vmem = pl.BlockSpec(memory_space=pltpu.VMEM)
    bf16, f32 = jnp.bfloat16, jnp.float32
    return pl.pallas_call(
        body,
        out_shape=jax.ShapeDtypeStruct((4, 2 * ANG, depth), bf16),
        in_specs=[pl.BlockSpec(memory_space=pltpu.SMEM)]
        + [vmem] * 4
        + [pl.BlockSpec(memory_space=pl.ANY)],
        out_specs=vmem,
        scratch_shapes=[
            pltpu.VMEM((block_count, 2, inner, depth), bf16),
            pltpu.VMEM((16, groups, inner, LANES), bf16),
            pltpu.VMEM((16, groups, inner, LANES), bf16),
            pltpu.VMEM((ROWS, PLACES, LANES), f32),
            pltpu.VMEM((16 * SLOTS * ROWS, LANES), f32),
            pltpu.VMEM((PLACES, 16 * SLOTS), bf16),
            pltpu.VMEM((16 * SLOTS, LANES), f32),
            pltpu.VMEM((16 * SLOTS, 2 * LANES), bf16),
            pltpu.VMEM((16 * SLOTS, 2 * LANES), bf16),
            pltpu.VMEM((4 * rounds, LANES), bf16),
            pltpu.VMEM((16, 4 * rounds, LANES), bf16),
            pltpu.VMEM((2, rounds, 16 * SLOTS), f32),
            pltpu.VMEM((8, ROWS, 64, LANES), bf16),
            pltpu.VMEM((8, ROWS, 64, LANES), bf16),
            pltpu.VMEM((2, 4, 4, ROWS, 16, LANES), bf16),
            pltpu.VMEM((2, 4, 4, ROWS, 16, LANES), bf16),
            pltpu.VMEM((ROWS * 16, LANES), f32),
            pltpu.VMEM((4, 16, ROWS, LANES), bf16),
            pltpu.VMEM((16, 4, ROWS, LANES), bf16),
            pltpu.VMEM((4, 8, LANES), f32),
            pltpu.VMEM((23, 8, LANES), f32),
            dma((rounds, WAYS)),
            dma((rounds, 15)),
            dma((rounds, 15)),
            dma((15,)),
            dma((15,)),
            dma((8,)),
            dma((8,)),
            dma((2, 4, 4)),
            dma((2, 4, 4)),
            dma((15,)),
            dma((15,)),
            dma((23,)),
            dma((23,)),
        ],
        compiler_params=pltpu.CompilerParams(
            collective_id=1, has_side_effects=True, vmem_limit_bytes=66 * 10**6
        ),
    )(
        jnp.sum(live, axis=1),
        live.T,
        block_tile.reshape(1, block_count),
        image_slot.reshape(1, block_count),
        slant_weights.T,
        offsets.reshape(block_count, 2, inner, depth),
    )


def solution(mesh):
    torus = Mesh(mesh.devices.reshape(4, 8, 2, mesh.shape["grp"]), SHOT_GRP)
    return jax.shard_map(
        local,
        mesh=torus,
        in_specs=(P(SHOT_GRP, None, None), P(), P(SHOT_GRP, None), P(SHOT_GRP, None), P(SHOT_GRP)),
        out_specs=P(SHOT_GRP, None, None),
        check_vma=False,
    )
```

```python
import functools

import jax
import jax.numpy as jnp
from jax import lax
from jax.experimental import pallas as pl
from jax.experimental.pallas import tpu as pltpu
from jax.sharding import Mesh
from jax.sharding import PartitionSpec as P

SHOT_GRP = ("y", "z", "c", "x")
ANG = 64
LANES = 128
WAYS = 4
DEPTHS = LANES // WAYS
ROWS = ANG // WAYS
ROUND = 4
SLOTS = WAYS * ROUND
PHASES = 2
PLACES = 1024
TILE = 256
MESH = pl.DeviceIdType.MESH
STEPS = (
    (1, 0), (3, 0), (0, 1), (0, 3), (1, 1), (3, 3), (1, 3), (3, 1),
    (2, 0), (0, 2), (2, 1), (1, 2), (2, 3), (3, 2), (2, 2),
)
UP_ORDER = (2, 3, 0, 1)
DOWN_ORDER = (0, 1, 2, 3)
EXACT = lax.Precision.HIGHEST


def exact_dot(a, b, dims):
    return lax.dot_general(
        a, b, (dims, ((), ())), precision=EXACT, preferred_element_type=jnp.float32
    )


def body(
    cut_ref,
    live_ref,
    tile_ref,
    slot_ref,
    weight_ref,
    offset_hbm,
    out_ref,
    held,
    sent,
    raw,
    acc,
    angles,
    chosen,
    cut_rows,
    even_side,
    odd_side,
    note,
    notes,
    note_sums,
    other,
    got,
    ring_out,
    ring_in,
    turned,
    last,
    landed,
    sums,
    sums_in,
    load_sem,
    send_sem,
    recv_sem,
    note_send,
    note_recv,
    swap_send,
    swap_recv,
    ring_send,
    ring_recv,
    last_send,
    last_recv,
    sums_send,
    sums_recv,
):
    x, y = lax.axis_index("x"), lax.axis_index("y")
    z, c = lax.axis_index("z"), lax.axis_index("c")
    me = x * 4 + y
    spread = [{"x": lax.rem(x + dx, 4), "y": lax.rem(y + dy, 4)} for dx, dy in STEPS]
    column = [{"z": lax.rem(z + step, 8)} for step in range(1, 8)]
    ring = (column[0], column[-1])
    partner = {"c": 1 - c}
    groups = held.shape[0] // WAYS
    rounds = groups // ROUND
    block_count, positions = tile_ref.shape[1], live_ref.shape[1]
    depth = held.shape[-1]

    def remote(source, target, send, recv, peer):
        return pltpu.make_async_remote_copy(
            src_ref=source,
            dst_ref=target,
            send_sem=send,
            recv_sem=recv,
            device_id=peer,
            device_id_type=MESH,
        )

    def load(turn, way):
        at = pl.ds(way * groups + turn * ROUND, ROUND)
        return pltpu.make_async_copy(offset_hbm.at[at], held.at[at], load_sem.at[turn, way])

    def start_loads(turn, carry):
        for way in range(WAYS):
            load(turn, way).start()
        return carry

    lax.fori_loop(0, rounds, start_loads, 0)

    tile, slot = tile_ref[...], slot_ref[...]
    code = ((tile & 1) ^ c) * 512 + ((((tile >> 1) & 7) - z + 8) & 7) * 64
    code = code + (slot >> 2) * 16 + (tile >> 4) * 4 + (slot & 3) + 1
    live = live_ref[...].astype(jnp.float32)
    position = lax.broadcasted_iota(jnp.int32, (positions, block_count), 0)
    block = lax.broadcasted_iota(jnp.int32, (positions, block_count), 1)
    live_cuts = jnp.broadcast_to(jnp.sum(live, axis=0, keepdims=True), (8, positions))
    values = [(code >> 5).astype(jnp.float32), (code & 31).astype(jnp.float32)]
    for place in range(2):
        pick = jnp.where(position == 2 * block + place, 1.0, 0.0)
        values.append(exact_dot(live_cuts, pick, ((1,), (0,)))[:1])
    turn_of = lax.broadcasted_iota(jnp.int32, (8, block_count), 1) % groups // ROUND
    own_turn = lax.broadcasted_iota(jnp.int32, (8, block_count), 0)
    spot = lax.broadcasted_iota(jnp.int32, (block_count, LANES), 0)
    lane = lax.broadcasted_iota(jnp.int32, (block_count, LANES), 1)
    spot = spot // groups * ROUND + spot % groups % ROUND + (me & 7) * SLOTS
    move = jnp.where(spot == lane, 1.0, 0.0)
    rows = [
        exact_dot(
            jnp.where(turn_of == own_turn, jnp.broadcast_to(value, (8, block_count)), 0.0),
            move,
            ((1,), (0,)),
        )
        for value in values
    ]
    own_note = jnp.concatenate(rows, axis=0).astype(jnp.bfloat16)
    note[...] = own_note
    notes[me] = own_note
    weights = jnp.transpose(weight_ref[...].astype(jnp.float32)).astype(jnp.bfloat16)

    peers = [partner, *column, *spread]
    barrier = pltpu.get_barrier_semaphore()
    for peer in peers:
        pl.semaphore_signal(barrier, inc=1, device_id=peer, device_id_type=MESH)
    pl.semaphore_wait(barrier, len(peers))

    note_copies = [
        remote(note, notes.at[me], note_send.at[n], note_recv.at[n], peer)
        for n, peer in enumerate(spread)
    ]
    for copy in note_copies:
        copy.start()

    def copy(phase, turn, n):
        at = pl.ds(turn * ROUND, ROUND)
        peer = spread[n]
        return remote(
            sent.at[phase, peer["x"] * 4 + peer["y"], at],
            raw.at[phase, me, at],
            send_sem.at[phase, turn, n],
            recv_sem.at[phase, turn, n],
            peer,
        )

    def send(phase, turn):
        at = pl.ds(turn * ROUND, ROUND)
        for quarter in range(4):
            lanes = slice(quarter * LANES, (quarter + 1) * LANES)
            for place in range(2):
                parts = [
                    held[pl.ds(way * groups + turn * ROUND, ROUND), place, :, lanes]
                    for way in range(WAYS)
                ]
                for end in range(2):
                    low = (end * PHASES + phase) * DEPTHS
                    sent[phase, 4 * quarter + 2 * place + end, at] = jnp.concatenate(
                        [part[..., low : low + DEPTHS] for part in parts], axis=-1
                    )
        for n in range(len(spread)):
            copy(phase, turn, n).start()
        raw[phase, me, at] = sent[phase, me, at]

    def send_first(turn, carry):
        for way in range(WAYS):
            load(turn, way).wait()
        send(0, turn)
        return carry

    lax.fori_loop(0, rounds, send_first, 0)

    angle = lax.broadcasted_iota(jnp.int32, (ANG, LANES), 0)

    def square(i, total):
        for place in range(2):
            part = jnp.dot(weights, held[i, place], preferred_element_type=jnp.float32)
            squares = part * part
            folded = (squares[:, :128] + squares[:, 128:256]) + (
                squares[:, 256:384] + squares[:, 384:]
            )
            total = total + jnp.where(angle < cut_ref[2 * i + place], folded, 0.0)
        return total

    total = lax.fori_loop(0, held.shape[0], square, jnp.zeros((ANG, LANES), jnp.float32))
    along = ((1,), (1,))
    sums[0] = jnp.concatenate(
        [
            exact_dot(jnp.ones((8, LANES), jnp.float32), total, along),
            exact_dot(jnp.ones((8, positions), jnp.float32), live, along),
        ],
        axis=1,
    )
    sum_base = (0, 1, 16)
    sum_peers = ([partner], spread, column)

    def sum_start(stage):
        flying = []
        for n, peer in enumerate(sum_peers[stage], sum_base[stage]):
            flying.append(
                remote(sums.at[stage], sums_in.at[n], sums_send.at[n], sums_recv.at[n], peer)
            )
            flying[-1].start()
        return flying

    def sum_wait(stage, flying):
        for piece in flying:
            piece.wait()
        total = sums[stage]
        for n in range(len(flying)):
            total = total + sums_in[sum_base[stage] + n]
        sums[stage + 1] = total

    flying = sum_start(0)

    def clear(i, carry):
        acc[:, :, pl.ds(i * 8, 8)] = jnp.zeros((PHASES, ROWS, 8, LANES), jnp.float32)
        return carry

    lax.fori_loop(0, PLACES // 8, clear, 0)

    sum_wait(0, flying)
    flying = sum_start(1)
    for piece in note_copies:
        piece.wait()
    for half in range(2):
        total = notes[half * 8].astype(jnp.float32)
        for n in range(1, 8):
            total = total + notes[half * 8 + n].astype(jnp.float32)
        high, low, near, far = total[:8], total[8:16], total[16:24], total[24:]
        note_sums[0, :, half * LANES : (half + 1) * LANES] = high * 32.0 + low
        note_sums[1, :, half * LANES : (half + 1) * LANES] = jnp.where(y < 2, near, far)

    tile_group = lax.broadcasted_iota(jnp.int32, (ROWS, LANES), 1) // DEPTHS
    lane_group = lax.broadcasted_iota(jnp.int32, (16 * SLOTS, LANES), 1) // DEPTHS
    together = 4

    def stack(phase, turn, carry):
        for n in range(len(spread)):
            copy(phase, turn, n).wait()
        if phase + 1 < PHASES:
            send(phase + 1, turn)

        def slant(i, inner_carry):
            rows = []
            for u in range(together):
                for n in range(ROUND):
                    rows.append(raw[phase, i * together + u, turn * ROUND + n])
            part = jnp.dot(
                weights, jnp.concatenate(rows, axis=1), preferred_element_type=jnp.float32
            )
            for u in range(together):
                for n in range(ROUND):
                    at = (u * ROUND + n) * LANES
                    row = part[:, at : at + LANES]
                    moved = [row] + [
                        pltpu.roll(row, LANES - t * DEPTHS, 1) for t in range(1, WAYS)
                    ]
                    for way in range(WAYS):
                        block = moved[way][:ROWS]
                        for group in range(1, WAYS):
                            piece = moved[(way - group) % WAYS]
                            piece = piece[group * ROWS : (group + 1) * ROWS]
                            block = jnp.where(tile_group == group, piece, block)
                        base = ((i * together + u) * SLOTS + way * ROUND + n) * ROWS
                        angles[pl.ds(base, ROWS)] = block
            return inner_carry

        lax.fori_loop(0, 16 // together, slant, 0)

        codes = note_sums[0, pl.ds(turn, 1), :]

        def choose(i, inner_carry):
            place = lax.broadcasted_iota(jnp.int32, (64, 16 * SLOTS), 0) + (i * 64 + 1)
            same = place.astype(jnp.float32) == codes
            chosen[pl.ds(i * 64, 64)] = jnp.where(same, 1.0, 0.0).astype(jnp.bfloat16)
            return inner_carry

        lax.fori_loop(0, PLACES // 64, choose, 0)
        mark = lax.broadcasted_iota(jnp.int32, (8, LANES), 0) == turn
        cut = exact_dot(
            note_sums[1], jnp.where(mark, 1.0, 0.0).astype(jnp.float32), ((0,), (0,))
        )
        cut_rows[...] = cut - (lane_group * ROWS).astype(jnp.float32)

        def gather(pair, side):
            for n in range(2):
                r = 2 * pair + n
                part = angles[pl.ds(r, 16 * SLOTS, stride=ROWS), :]
                keep = cut_rows[...] > lax.convert_element_type(r, jnp.float32)
                side[:, n * LANES : (n + 1) * LANES] = jnp.where(keep, part, 0.0).astype(
                    jnp.bfloat16
                )

        def product(pair, side):
            value = side[...]
            for n in range(PLACES // TILE):
                at = pl.ds(n * TILE, TILE)
                part = jnp.dot(chosen[at], value, preferred_element_type=jnp.float32)
                acc[phase, 2 * pair, at] += part[:, :LANES]
                acc[phase, 2 * pair + 1, at] += part[:, LANES:]

        gather(0, even_side)

        def add(i, inner_carry):
            gather(2 * i + 1, odd_side)
            product(2 * i, even_side)
            gather(jnp.minimum(2 * i + 2, ROWS // 2 - 1), even_side)
            product(2 * i + 1, odd_side)
            return inner_carry

        lax.fori_loop(0, ROWS // 4, add, 0)
        return carry

    def run(phase, first, end):
        lax.fori_loop(first, end, functools.partial(stack, phase), 0)

    swaps, copies = {}, {}

    def swap(phase):
        for chunk in (4, 3, 5, 2, 6, 1, 7, 0):
            half = acc[phase, :, 512 + chunk * 64 : 512 + (chunk + 1) * 64]
            other[phase, chunk] = half.astype(jnp.bfloat16)
            swaps[phase, chunk] = remote(
                other.at[phase, chunk],
                got.at[phase, chunk],
                swap_send.at[phase, chunk],
                swap_recv.at[phase, chunk],
                partner,
            )
            swaps[phase, chunk].start()

    def own(phase, chunk, part):
        at = chunk * 64 + part * 16
        theirs = got[phase, chunk, :, part * 16 : (part + 1) * 16]
        return acc[phase, :, at : at + 16] + theirs.astype(jnp.float32)

    def ring_step(phase, step):
        for chunk in ((4,), (3, 5), (2, 6), (1, 7))[step]:
            swaps[phase, chunk].wait()
        for number in range(4):
            for way, order in enumerate((UP_ORDER, DOWN_ORDER)):
                if step == 0 and number < 2:
                    continue
                part = order[number]
                value = own(phase, 4 - step if way == 0 else 4 + step, part)
                before = copies.get((phase, way, step - 1, part))
                if before is not None:
                    before.wait_recv()
                    value = value + ring_in[phase, way, step - 1, part].astype(jnp.float32)
                ring_out[phase, way, step, part] = value.astype(jnp.bfloat16)
                piece = remote(
                    ring_out.at[phase, way, step, part],
                    ring_in.at[phase, way, step, part],
                    ring_send.at[phase, way, step, part],
                    ring_recv.at[phase, way, step, part],
                    ring[way],
                )
                piece.start()
                copies[phase, way, step, part] = piece

    def deliver(phase, gain):
        swaps[phase, 0].wait()
        for part in (2, 0, 3, 1):
            value = own(phase, 0, part)
            for way in range(2):
                copies[phase, way, 3, part].wait_recv()
                value = value + ring_in[phase, way, 3, part].astype(jnp.float32)
            turned[...] = value.reshape(ROWS * 16, LANES)
            for n in range(16):
                rows = turned[pl.ds(n, ROWS, stride=16), :]
                last[phase, part, n] = (rows * gain).astype(jnp.bfloat16)
        ends = []
        for n, peer in enumerate(spread):
            piece = remote(
                last.at[phase, peer["x"], pl.ds(peer["y"] * 4, 4)],
                landed.at[phase, me],
                last_send.at[phase, n],
                last_recv.at[phase, n],
                peer,
            )
            piece.start()
            ends.append(piece)
        landed[phase, me] = last[phase, x, pl.ds(y * 4, 4)]
        return ends

    run(0, 0, rounds)
    swap(0)
    sum_wait(1, flying)
    flying = sum_start(2)
    ring_step(0, 0)
    run(1, 0, 1)
    ring_step(0, 1)
    run(1, 1, 3)
    ring_step(0, 2)
    sum_wait(2, flying)
    run(1, 3, 4)
    ring_step(0, 3)
    totals = sums[3]
    gain = lax.rsqrt(totals[:, :ANG] / (depth * totals[:, ANG:]) + 1e-06)
    angle = lax.broadcasted_iota(jnp.int32, (ROWS, ANG), 1)
    row = lax.broadcasted_iota(jnp.int32, (ROWS, ANG), 0)
    picked = jnp.where(angle % ROWS == row, jnp.broadcast_to(gain[:1], (ROWS, ANG)), 0.0)
    angle = lax.broadcasted_iota(jnp.int32, (ANG, LANES), 0)
    lane = lax.broadcasted_iota(jnp.int32, (ANG, LANES), 1)
    gain = exact_dot(
        picked, jnp.where(angle // ROWS == lane // DEPTHS, 1.0, 0.0), ((1,), (0,))
    )
    run(1, 4, 5)
    ends = deliver(0, gain)
    run(1, 5, rounds)
    swap(1)
    for step in range(4):
        ring_step(1, step)
    ends = ends + deliver(1, gain)
    for piece in copies.values():
        piece.wait_send()
    for piece in ends:
        piece.wait()
    for slot in range(4):
        for quarter in range(4):
            lanes = slice(quarter * LANES, (quarter + 1) * LANES)
            for place in range(2):
                parts = [
                    landed[phase, 4 * quarter + 2 * place + end, slot]
                    for end in range(2)
                    for phase in range(PHASES)
                ]
                for group in range(WAYS):
                    at = place * ANG + group * ROWS
                    cut = slice(group * DEPTHS, (group + 1) * DEPTHS)
                    out_ref[slot, at : at + ROWS, lanes] = jnp.concatenate(
                        [part[:, cut] for part in parts], axis=1
                    )


def local(offsets, slant_weights, live, block_tile, image_slot):
    block_count = block_tile.shape[0]
    positions, inner, depth = offsets.shape
    groups = block_count // WAYS
    rounds = groups // ROUND
    dma = pltpu.SemaphoreType.DMA
    vmem = pl.BlockSpec(memory_space=pltpu.VMEM)
    bf16, f32 = jnp.bfloat16, jnp.float32
    return pl.pallas_call(
        body,
        out_shape=jax.ShapeDtypeStruct((4, 2 * ANG, depth), bf16),
        in_specs=[pl.BlockSpec(memory_space=pltpu.SMEM)]
        + [vmem] * 4
        + [pl.BlockSpec(memory_space=pl.ANY)],
        out_specs=vmem,
        scratch_shapes=[
            pltpu.VMEM((block_count, 2, inner, depth), bf16),
            pltpu.VMEM((PHASES, 16, groups, inner, LANES), bf16),
            pltpu.VMEM((PHASES, 16, groups, inner, LANES), bf16),
            pltpu.VMEM((PHASES, ROWS, PLACES, LANES), f32),
            pltpu.VMEM((16 * SLOTS * ROWS, LANES), f32),
            pltpu.VMEM((PLACES, 16 * SLOTS), bf16),
            pltpu.VMEM((16 * SLOTS, LANES), f32),
            pltpu.VMEM((16 * SLOTS, 2 * LANES), bf16),
            pltpu.VMEM((16 * SLOTS, 2 * LANES), bf16),
            pltpu.VMEM((32, LANES), bf16),
            pltpu.VMEM((16, 32, LANES), bf16),
            pltpu.VMEM((2, 8, 16 * SLOTS), f32),
            pltpu.VMEM((PHASES, 8, ROWS, 64, LANES), bf16),
            pltpu.VMEM((PHASES, 8, ROWS, 64, LANES), bf16),
            pltpu.VMEM((PHASES, 2, 4, 4, ROWS, 16, LANES), bf16),
            pltpu.VMEM((PHASES, 2, 4, 4, ROWS, 16, LANES), bf16),
            pltpu.VMEM((ROWS * 16, LANES), f32),
            pltpu.VMEM((PHASES, 4, 16, ROWS, LANES), bf16),
            pltpu.VMEM((PHASES, 16, 4, ROWS, LANES), bf16),
            pltpu.VMEM((4, 8, LANES), f32),
            pltpu.VMEM((23, 8, LANES), f32),
            dma((rounds, WAYS)),
            dma((PHASES, rounds, 15)),
            dma((PHASES, rounds, 15)),
            dma((15,)),
            dma((15,)),
            dma((PHASES, 8)),
            dma((PHASES, 8)),
            dma((PHASES, 2, 4, 4)),
            dma((PHASES, 2, 4, 4)),
            dma((PHASES, 15)),
            dma((PHASES, 15)),
            dma((23,)),
            dma((23,)),
        ],
        compiler_params=pltpu.CompilerParams(
            collective_id=1, has_side_effects=True, vmem_limit_bytes=66 * 10**6
        ),
    )(
        jnp.sum(live, axis=1),
        live.T,
        block_tile.reshape(1, block_count),
        image_slot.reshape(1, block_count),
        slant_weights.T,
        offsets.reshape(block_count, 2, inner, depth),
    )


def solution(mesh):
    torus = Mesh(mesh.devices.reshape(4, 8, 2, mesh.shape["grp"]), SHOT_GRP)
    return jax.shard_map(
        local,
        mesh=torus,
        in_specs=(P(SHOT_GRP, None, None), P(), P(SHOT_GRP, None), P(SHOT_GRP, None), P(SHOT_GRP)),
        out_specs=P(SHOT_GRP, None, None),
        check_vma=False,
    )
```

```python
import functools

import jax
import jax.numpy as jnp
from jax import lax
from jax.experimental import pallas as pl
from jax.experimental.pallas import tpu as pltpu
from jax.sharding import Mesh
from jax.sharding import PartitionSpec as P

SHOT_GRP = ("y", "z", "c", "x")
ANG = 64
LANES = 128
WAYS = 4
DEPTHS = LANES // WAYS
ROWS = ANG // WAYS
ROUND = 4
SLOTS = WAYS * ROUND
PHASES = 2
PLACES = 1024
TILE = 256
MESH = pl.DeviceIdType.MESH
STEPS = (
    (1, 0), (3, 0), (0, 1), (0, 3), (1, 1), (3, 3), (1, 3), (3, 1),
    (2, 0), (0, 2), (2, 1), (1, 2), (2, 3), (3, 2), (2, 2),
)
UP_ORDER = (2, 3, 0, 1)
DOWN_ORDER = (0, 1, 2, 3)
EXACT = lax.Precision.HIGHEST


def exact_dot(a, b, dims):
    return lax.dot_general(
        a, b, (dims, ((), ())), precision=EXACT, preferred_element_type=jnp.float32
    )


def body(
    cut_ref,
    live_ref,
    tile_ref,
    slot_ref,
    weight_ref,
    offset_hbm,
    out_ref,
    held,
    sent,
    raw,
    acc,
    angles,
    chosen,
    cut_rows,
    even_side,
    odd_side,
    note,
    notes,
    note_sums,
    other,
    got,
    ring_out,
    ring_in,
    turned,
    last,
    landed,
    sums,
    sums_in,
    load_sem,
    send_sem,
    recv_sem,
    note_send,
    note_recv,
    swap_send,
    swap_recv,
    ring_send,
    ring_recv,
    last_send,
    last_recv,
    sums_send,
    sums_recv,
):
    x, y = lax.axis_index("x"), lax.axis_index("y")
    z, c = lax.axis_index("z"), lax.axis_index("c")
    me = x * 4 + y
    spread = [{"x": lax.rem(x + dx, 4), "y": lax.rem(y + dy, 4)} for dx, dy in STEPS]
    column = [{"z": lax.rem(z + step, 8)} for step in range(1, 8)]
    ring = (column[0], column[-1])
    partner = {"c": 1 - c}
    groups = held.shape[0] // WAYS
    rounds = groups // ROUND
    block_count, positions = tile_ref.shape[1], live_ref.shape[1]
    depth = held.shape[-1]

    def remote(source, target, send, recv, peer):
        return pltpu.make_async_remote_copy(
            src_ref=source,
            dst_ref=target,
            send_sem=send,
            recv_sem=recv,
            device_id=peer,
            device_id_type=MESH,
        )

    def load(turn, way):
        at = pl.ds(way * groups + turn * ROUND, ROUND)
        return pltpu.make_async_copy(offset_hbm.at[at], held.at[at], load_sem.at[turn, way])

    def start_loads(turn, carry):
        for way in range(WAYS):
            load(turn, way).start()
        return carry

    lax.fori_loop(0, rounds, start_loads, 0)

    tile, slot = tile_ref[...], slot_ref[...]
    code = ((tile & 1) ^ c) * 512 + ((((tile >> 1) & 7) - z + 8) & 7) * 64
    code = code + (slot >> 2) * 16 + (tile >> 4) * 4 + (slot & 3) + 1
    live = live_ref[...].astype(jnp.float32)
    position = lax.broadcasted_iota(jnp.int32, (positions, block_count), 0)
    block = lax.broadcasted_iota(jnp.int32, (positions, block_count), 1)
    live_cuts = jnp.broadcast_to(jnp.sum(live, axis=0, keepdims=True), (8, positions))
    values = [(code >> 5).astype(jnp.float32), (code & 31).astype(jnp.float32)]
    for place in range(2):
        pick = jnp.where(position == 2 * block + place, 1.0, 0.0)
        values.append(exact_dot(live_cuts, pick, ((1,), (0,)))[:1])
    turn_of = lax.broadcasted_iota(jnp.int32, (8, block_count), 1) % groups // ROUND
    own_turn = lax.broadcasted_iota(jnp.int32, (8, block_count), 0)
    spot = lax.broadcasted_iota(jnp.int32, (block_count, LANES), 0)
    lane = lax.broadcasted_iota(jnp.int32, (block_count, LANES), 1)
    spot = spot // groups * ROUND + spot % groups % ROUND + (me & 7) * SLOTS
    move = jnp.where(spot == lane, 1.0, 0.0)
    rows = [
        exact_dot(
            jnp.where(turn_of == own_turn, jnp.broadcast_to(value, (8, block_count)), 0.0),
            move,
            ((1,), (0,)),
        )
        for value in values
    ]
    own_note = jnp.concatenate(rows, axis=0).astype(jnp.bfloat16)
    note[...] = own_note
    notes[me] = own_note
    weights = jnp.transpose(weight_ref[...].astype(jnp.float32)).astype(jnp.bfloat16)

    peers = [partner, *column, *spread]
    barrier = pltpu.get_barrier_semaphore()
    for peer in peers:
        pl.semaphore_signal(barrier, inc=1, device_id=peer, device_id_type=MESH)
    pl.semaphore_wait(barrier, len(peers))

    note_copies = [
        remote(note, notes.at[me], note_send.at[n], note_recv.at[n], peer)
        for n, peer in enumerate(spread)
    ]
    for copy in note_copies:
        copy.start()

    def copy(phase, turn, n):
        at = pl.ds(turn * ROUND, ROUND)
        peer = spread[n]
        return remote(
            sent.at[phase, peer["x"] * 4 + peer["y"], at],
            raw.at[phase, me, at],
            send_sem.at[phase, turn, n],
            recv_sem.at[phase, turn, n],
            peer,
        )

    def send(phase, turn):
        at = pl.ds(turn * ROUND, ROUND)
        for quarter in range(4):
            lanes = slice(quarter * LANES, (quarter + 1) * LANES)
            for place in range(2):
                parts = [
                    held[pl.ds(way * groups + turn * ROUND, ROUND), place, :, lanes]
                    for way in range(WAYS)
                ]
                for end in range(2):
                    low = (end * PHASES + phase) * DEPTHS
                    sent[phase, 4 * quarter + 2 * place + end, at] = jnp.concatenate(
                        [part[..., low : low + DEPTHS] for part in parts], axis=-1
                    )
        for n in range(len(spread)):
            copy(phase, turn, n).start()
        raw[phase, me, at] = sent[phase, me, at]

    def send_first(turn, carry):
        for way in range(WAYS):
            load(turn, way).wait()
        send(0, turn)
        return carry

    lax.fori_loop(0, rounds, send_first, 0)

    angle = lax.broadcasted_iota(jnp.int32, (ANG, LANES), 0)

    def square(i, total):
        for place in range(2):
            part = jnp.dot(weights, held[i, place], preferred_element_type=jnp.float32)
            squares = part * part
            folded = (squares[:, :128] + squares[:, 128:256]) + (
                squares[:, 256:384] + squares[:, 384:]
            )
            total = total + jnp.where(angle < cut_ref[2 * i + place], folded, 0.0)
        return total

    total = lax.fori_loop(0, held.shape[0], square, jnp.zeros((ANG, LANES), jnp.float32))
    along = ((1,), (1,))
    sums[0] = jnp.concatenate(
        [
            exact_dot(jnp.ones((8, LANES), jnp.float32), total, along),
            exact_dot(jnp.ones((8, positions), jnp.float32), live, along),
        ],
        axis=1,
    )
    sum_base = (0, 1, 16)
    sum_peers = ([partner], spread, column)

    def sum_start(stage):
        flying = []
        for n, peer in enumerate(sum_peers[stage], sum_base[stage]):
            flying.append(
                remote(sums.at[stage], sums_in.at[n], sums_send.at[n], sums_recv.at[n], peer)
            )
            flying[-1].start()
        return flying

    def sum_wait(stage, flying):
        for piece in flying:
            piece.wait()
        total = sums[stage]
        for n in range(len(flying)):
            total = total + sums_in[sum_base[stage] + n]
        sums[stage + 1] = total

    flying = sum_start(0)

    def clear(i, carry):
        acc[:, :, pl.ds(i * 8, 8)] = jnp.zeros((PHASES, ROWS, 8, LANES), jnp.float32)
        return carry

    lax.fori_loop(0, PLACES // 8, clear, 0)

    sum_wait(0, flying)
    flying = sum_start(1)
    for piece in note_copies:
        piece.wait()
    for half in range(2):
        total = notes[half * 8].astype(jnp.float32)
        for n in range(1, 8):
            total = total + notes[half * 8 + n].astype(jnp.float32)
        high, low, near, far = total[:8], total[8:16], total[16:24], total[24:]
        note_sums[0, :, half * LANES : (half + 1) * LANES] = high * 32.0 + low
        note_sums[1, :, half * LANES : (half + 1) * LANES] = jnp.where(y < 2, near, far)

    row_group = lax.broadcasted_iota(jnp.int32, (raw.shape[3], LANES), 1) // DEPTHS
    side_by_side = jnp.concatenate(
        [weights[group * ROWS : (group + 1) * ROWS] for group in range(WAYS)], axis=1
    )
    lane_group = lax.broadcasted_iota(jnp.int32, (16 * SLOTS, LANES), 1) // DEPTHS
    together = 4

    def stack(phase, turn, carry):
        for n in range(len(spread)):
            copy(phase, turn, n).wait()
        if phase + 1 < PHASES:
            send(phase + 1, turn)

        def slant(i, inner_carry):
            tiles = []
            for u in range(together):
                for n in range(ROUND):
                    row = raw[phase, i * together + u, turn * ROUND + n]
                    moved = [row] + [
                        jnp.concatenate([row[:, t * DEPTHS :], row[:, : t * DEPTHS]], axis=1)
                        for t in range(1, WAYS)
                    ]
                    for way in range(WAYS):
                        parts = [
                            jnp.where(row_group == group, moved[(way - group) % WAYS], 0)
                            for group in range(WAYS)
                        ]
                        tiles.append(jnp.concatenate(parts, axis=0).astype(jnp.bfloat16))
            part = jnp.dot(
                side_by_side,
                jnp.concatenate(tiles, axis=1),
                preferred_element_type=jnp.float32,
            )
            for n in range(len(tiles)):
                u, place = n // SLOTS, n % SLOTS
                at = u * SLOTS + place % WAYS * ROUND + place // WAYS
                base = (i * together * SLOTS + at) * ROWS
                angles[pl.ds(base, ROWS)] = part[:, n * LANES : (n + 1) * LANES]
            return inner_carry

        lax.fori_loop(0, 16 // together, slant, 0)

        codes = note_sums[0, pl.ds(turn, 1), :]

        def choose(i, inner_carry):
            place = lax.broadcasted_iota(jnp.int32, (64, 16 * SLOTS), 0) + (i * 64 + 1)
            same = place.astype(jnp.float32) == codes
            chosen[pl.ds(i * 64, 64)] = jnp.where(same, 1.0, 0.0).astype(jnp.bfloat16)
            return inner_carry

        lax.fori_loop(0, PLACES // 64, choose, 0)
        mark = lax.broadcasted_iota(jnp.int32, (8, LANES), 0) == turn
        cut = exact_dot(
            note_sums[1], jnp.where(mark, 1.0, 0.0).astype(jnp.float32), ((0,), (0,))
        )
        cut_rows[...] = cut - (lane_group * ROWS).astype(jnp.float32)

        def gather(pair, side):
            for n in range(2):
                r = 2 * pair + n
                part = angles[pl.ds(r, 16 * SLOTS, stride=ROWS), :]
                keep = cut_rows[...] > lax.convert_element_type(r, jnp.float32)
                side[:, n * LANES : (n + 1) * LANES] = jnp.where(keep, part, 0.0).astype(
                    jnp.bfloat16
                )

        def product(pair, side):
            value = side[...]
            for n in range(PLACES // TILE):
                at = pl.ds(n * TILE, TILE)
                part = jnp.dot(chosen[at], value, preferred_element_type=jnp.float32)
                acc[phase, 2 * pair, at] += part[:, :LANES]
                acc[phase, 2 * pair + 1, at] += part[:, LANES:]

        gather(0, even_side)

        def add(i, inner_carry):
            gather(2 * i + 1, odd_side)
            product(2 * i, even_side)
            gather(jnp.minimum(2 * i + 2, ROWS // 2 - 1), even_side)
            product(2 * i + 1, odd_side)
            return inner_carry

        lax.fori_loop(0, ROWS // 4, add, 0)
        return carry

    def run(phase, first, end):
        lax.fori_loop(first, end, functools.partial(stack, phase), 0)

    swaps, copies = {}, {}

    def swap(phase):
        for chunk in (4, 3, 5, 2, 6, 1, 7, 0):
            half = acc[phase, :, 512 + chunk * 64 : 512 + (chunk + 1) * 64]
            other[phase, chunk] = half.astype(jnp.bfloat16)
            swaps[phase, chunk] = remote(
                other.at[phase, chunk],
                got.at[phase, chunk],
                swap_send.at[phase, chunk],
                swap_recv.at[phase, chunk],
                partner,
            )
            swaps[phase, chunk].start()

    def own(phase, chunk, part):
        at = chunk * 64 + part * 16
        theirs = got[phase, chunk, :, part * 16 : (part + 1) * 16]
        return acc[phase, :, at : at + 16] + theirs.astype(jnp.float32)

    def ring_step(phase, step):
        for chunk in ((4,), (3, 5), (2, 6), (1, 7))[step]:
            swaps[phase, chunk].wait()
        for number in range(4):
            for way, order in enumerate((UP_ORDER, DOWN_ORDER)):
                if step == 0 and number < 2:
                    continue
                part = order[number]
                value = own(phase, 4 - step if way == 0 else 4 + step, part)
                before = copies.get((phase, way, step - 1, part))
                if before is not None:
                    before.wait_recv()
                    value = value + ring_in[phase, way, step - 1, part].astype(jnp.float32)
                ring_out[phase, way, step, part] = value.astype(jnp.bfloat16)
                piece = remote(
                    ring_out.at[phase, way, step, part],
                    ring_in.at[phase, way, step, part],
                    ring_send.at[phase, way, step, part],
                    ring_recv.at[phase, way, step, part],
                    ring[way],
                )
                piece.start()
                copies[phase, way, step, part] = piece

    def deliver(phase, gain):
        swaps[phase, 0].wait()
        for part in (2, 0, 3, 1):
            value = own(phase, 0, part)
            for way in range(2):
                copies[phase, way, 3, part].wait_recv()
                value = value + ring_in[phase, way, 3, part].astype(jnp.float32)
            turned[...] = value.reshape(ROWS * 16, LANES)
            for n in range(16):
                rows = turned[pl.ds(n, ROWS, stride=16), :]
                last[phase, part, n] = (rows * gain).astype(jnp.bfloat16)
        ends = []
        for n, peer in enumerate(spread):
            piece = remote(
                last.at[phase, peer["x"], pl.ds(peer["y"] * 4, 4)],
                landed.at[phase, me],
                last_send.at[phase, n],
                last_recv.at[phase, n],
                peer,
            )
            piece.start()
            ends.append(piece)
        landed[phase, me] = last[phase, x, pl.ds(y * 4, 4)]
        return ends

    run(0, 0, rounds)
    swap(0)
    sum_wait(1, flying)
    flying = sum_start(2)
    ring_step(0, 0)
    run(1, 0, 1)
    ring_step(0, 1)
    run(1, 1, 3)
    ring_step(0, 2)
    sum_wait(2, flying)
    run(1, 3, 4)
    ring_step(0, 3)
    totals = sums[3]
    gain = lax.rsqrt(totals[:, :ANG] / (depth * totals[:, ANG:]) + 1e-06)
    angle = lax.broadcasted_iota(jnp.int32, (ROWS, ANG), 1)
    row = lax.broadcasted_iota(jnp.int32, (ROWS, ANG), 0)
    picked = jnp.where(angle % ROWS == row, jnp.broadcast_to(gain[:1], (ROWS, ANG)), 0.0)
    angle = lax.broadcasted_iota(jnp.int32, (ANG, LANES), 0)
    lane = lax.broadcasted_iota(jnp.int32, (ANG, LANES), 1)
    gain = exact_dot(
        picked, jnp.where(angle // ROWS == lane // DEPTHS, 1.0, 0.0), ((1,), (0,))
    )
    run(1, 4, 5)
    ends = deliver(0, gain)
    run(1, 5, rounds)
    swap(1)
    for step in range(4):
        ring_step(1, step)
    ends = ends + deliver(1, gain)
    for piece in copies.values():
        piece.wait_send()
    for piece in ends:
        piece.wait()
    for slot in range(4):
        for quarter in range(4):
            lanes = slice(quarter * LANES, (quarter + 1) * LANES)
            for place in range(2):
                parts = [
                    landed[phase, 4 * quarter + 2 * place + end, slot]
                    for end in range(2)
                    for phase in range(PHASES)
                ]
                for group in range(WAYS):
                    at = place * ANG + group * ROWS
                    cut = slice(group * DEPTHS, (group + 1) * DEPTHS)
                    out_ref[slot, at : at + ROWS, lanes] = jnp.concatenate(
                        [part[:, cut] for part in parts], axis=1
                    )


def local(offsets, slant_weights, live, block_tile, image_slot):
    block_count = block_tile.shape[0]
    positions, inner, depth = offsets.shape
    groups = block_count // WAYS
    rounds = groups // ROUND
    dma = pltpu.SemaphoreType.DMA
    vmem = pl.BlockSpec(memory_space=pltpu.VMEM)
    bf16, f32 = jnp.bfloat16, jnp.float32
    return pl.pallas_call(
        body,
        out_shape=jax.ShapeDtypeStruct((4, 2 * ANG, depth), bf16),
        in_specs=[pl.BlockSpec(memory_space=pltpu.SMEM)]
        + [vmem] * 4
        + [pl.BlockSpec(memory_space=pl.ANY)],
        out_specs=vmem,
        scratch_shapes=[
            pltpu.VMEM((block_count, 2, inner, depth), bf16),
            pltpu.VMEM((PHASES, 16, groups, inner, LANES), bf16),
            pltpu.VMEM((PHASES, 16, groups, inner, LANES), bf16),
            pltpu.VMEM((PHASES, ROWS, PLACES, LANES), f32),
            pltpu.VMEM((16 * SLOTS * ROWS, LANES), f32),
            pltpu.VMEM((PLACES, 16 * SLOTS), bf16),
            pltpu.VMEM((16 * SLOTS, LANES), f32),
            pltpu.VMEM((16 * SLOTS, 2 * LANES), bf16),
            pltpu.VMEM((16 * SLOTS, 2 * LANES), bf16),
            pltpu.VMEM((32, LANES), bf16),
            pltpu.VMEM((16, 32, LANES), bf16),
            pltpu.VMEM((2, 8, 16 * SLOTS), f32),
            pltpu.VMEM((PHASES, 8, ROWS, 64, LANES), bf16),
            pltpu.VMEM((PHASES, 8, ROWS, 64, LANES), bf16),
            pltpu.VMEM((PHASES, 2, 4, 4, ROWS, 16, LANES), bf16),
            pltpu.VMEM((PHASES, 2, 4, 4, ROWS, 16, LANES), bf16),
            pltpu.VMEM((ROWS * 16, LANES), f32),
            pltpu.VMEM((PHASES, 4, 16, ROWS, LANES), bf16),
            pltpu.VMEM((PHASES, 16, 4, ROWS, LANES), bf16),
            pltpu.VMEM((4, 8, LANES), f32),
            pltpu.VMEM((23, 8, LANES), f32),
            dma((rounds, WAYS)),
            dma((PHASES, rounds, 15)),
            dma((PHASES, rounds, 15)),
            dma((15,)),
            dma((15,)),
            dma((PHASES, 8)),
            dma((PHASES, 8)),
            dma((PHASES, 2, 4, 4)),
            dma((PHASES, 2, 4, 4)),
            dma((PHASES, 15)),
            dma((PHASES, 15)),
            dma((23,)),
            dma((23,)),
        ],
        compiler_params=pltpu.CompilerParams(
            collective_id=1, has_side_effects=True, vmem_limit_bytes=66 * 10**6
        ),
    )(
        jnp.sum(live, axis=1),
        live.T,
        block_tile.reshape(1, block_count),
        image_slot.reshape(1, block_count),
        slant_weights.T,
        offsets.reshape(block_count, 2, inner, depth),
    )


def solution(mesh):
    torus = Mesh(mesh.devices.reshape(4, 8, 2, mesh.shape["grp"]), SHOT_GRP)
    return jax.shard_map(
        local,
        mesh=torus,
        in_specs=(P(SHOT_GRP, None, None), P(), P(SHOT_GRP, None), P(SHOT_GRP, None), P(SHOT_GRP)),
        out_specs=P(SHOT_GRP, None, None),
        check_vma=False,
    )
```
